32 devices in a mesh: curve: 4 (over y, x), blk: 8 (over z, core).
Axes of the slice: x: 2, y: 2, z: 4, core: 2. Of those that a mesh axis runs over, the one named last changes fastest.
Arguments:
- anchors: bfloat16 [32768, 512], P(('curve', 'blk')), may hold values from -16 to 16
- keys: bfloat16 [4096, 512], P('blk'), may hold values from -16 to 16
- owners: int32 [32768, 1], P(('curve', 'blk')), may hold values from 0 to 7; in each aligned block of 1024 rows (0 to 1023, 1024 to 2047, ...) at most 256 rows name the same one
- key_rows: int32 [32768], P(('curve', 'blk')), may hold values from 0 to 511
Outputs:
- losses: float32 [32768], P(('curve', 'blk'))
- grad_anchors: float32 [32768, 512], P(('curve', 'blk'))
- lookup_derivative: float32 [4096, 512], P('blk')
The draws below stay inside these ranges and needn't reach their ends.
Inputs may be any that keep to these rules, and one draw needn't show every extreme that they name: `owners`: among the rows of one device at most 256 name the same bank, a bound that some block reaches of them.
All inputs are finite; a program needn't handle non-finite values.
Results may differ from the reference program's by a relative error of at most 0.0037.
Values may be sent and summed in bfloat16 or wider, within the bound.
No kernel may reach another device: no remote copies, remote signals or barrier semaphores. Data moves between devices by JAX's collectives and lax.ppermute only.
A program may use at most 64 MiB of HBM per device.

```python
import math
import jax
import jax.numpy as jnp
import numpy as np
from jax import lax

EMBED_WIDTH = 512
ROWS = 1024
STORE_ENTRY_TALLY = 512
STEPS = 4
CAP = 256
ANCH = 32768
KEYS = 4096
N_BLK = 8


kinds_total = 16


def scene_features(key, row_count, salt_value):
    protos = jax.random.normal(jax.random.fold_in(key, 101), (kinds_total, EMBED_WIDTH), jnp.float32)
    labels = jax.random.randint(jax.random.fold_in(key, salt_value), (row_count,), 0, kinds_total)
    jitter_key = jax.random.fold_in(key, salt_value + 1)
    jitter = jax.random.normal(jitter_key, (row_count, EMBED_WIDTH), jnp.float32)
    values = 2.0 * protos[labels] + jitter
    return jnp.clip(values, -16.0, 16.0)


def draw_anchors(key, part):
    return scene_features(key, ANCH, 11).astype(jnp.bfloat16)


def draw_keys(key, part):
    return scene_features(key, KEYS, 23).astype(jnp.bfloat16)


def set_ends(result, rng, low, top_value):
    longest = result.shape.index(max(result.shape))
    spots = []
    for shift in (0, 1):
        where = [jax.random.randint(jax.random.fold_in(rng, axis), (), 0, length) for axis, length in enumerate(result.shape)]
        where[longest] = (where[longest] + shift) % result.shape[longest]
        spots.append(tuple(where))
    return result.at[spots[0]].set(low).at[spots[1]].set(top_value)


def shared_out(rng, own, number, rows, number_of, top, limit, slope):
    sequence = jax.random.permutation(rng, number_of)
    heavy_load, usual = load_shares(number_of, rows * top, limit, slope, True), load_shares(number_of, rows * top, limit, slope, False)
    places = jnp.arange(number_of)

    def named(lengths, turn):
        used = int((lengths > 0).sum())
        fixed = max(1, used // 4)
        moved = fixed + (places - fixed + turn * (used - fixed)) % max(1, number_of - fixed)
        return jnp.zeros((number_of,), jnp.int32).at[sequence[jnp.where(places < fixed, places, moved)]].set(jnp.asarray(lengths, jnp.int32))

    lengths = jnp.where(number % 4 == 0, named(heavy_load, number // 4), named(usual, number - number // 4 - 1))
    mixed = jax.random.permutation(jax.random.fold_in(own, 3), number_of)
    donor, sink = mixed[0:number_of // 2 * 2:2], mixed[1:number_of // 2 * 2:2]
    room = jnp.minimum(lengths[donor] - 1, limit - lengths[sink]) // 2
    room = jnp.where((donor == sequence[0]) | (sink == sequence[0]) | (lengths[sink] == 0), 0, jnp.maximum(room, 0))
    moved = jax.random.randint(jax.random.fold_in(own, 4), (number_of // 2,), 0, 1 << 20) % (room + 1)
    lengths = lengths.at[donor].add(-moved).at[sink].add(moved)
    items = jnp.searchsorted(jnp.cumsum(lengths), jnp.arange(rows * top), side="right").astype(jnp.int32)
    listing = items.reshape(top, rows).T
    listing = listing[jax.random.permutation(jax.random.fold_in(own, 1), rows)]
    turn = jax.random.randint(jax.random.fold_in(own, 2), (rows, 1), 0, top)
    return jnp.take_along_axis(listing, (jnp.arange(top)[None, :] + turn) % top, axis=1)


def load_shares(number_of, total, reach, skew, full):
    portions = [(1 << 20) // math.isqrt(rank ** skew) + 1 for rank in range(1, number_of + 1)]
    largest = reach if full else min(reach, max(-(-total // number_of), total * portions[0] // sum(portions)))
    least = 1 if total - largest >= number_of - 1 else 0
    given, spare = [largest] + [least] * (number_of - 1), total - largest - least * (number_of - 1)
    while spare > 0:
        movable = [i for i in range(1, number_of) if given[i] < largest] or [i for i in range(1, number_of) if given[i] < reach]
        mass, budget = sum([portions[i] for i in movable]), spare
        for i in movable:
            extra = min(reach - given[i], max(1, budget * portions[i] // mass), spare)
            given[i] = given[i] + extra
            spare = spare - extra
    return np.array(given)


def setup_inputs(seed: int = 0) -> dict:
    key_list = jax.random.split(jax.random.key(seed), 5)
    anchors = draw_anchors(jax.random.fold_in(key_list[4], 71), 0)
    keys = draw_keys(jax.random.fold_in(key_list[4], 71), 0)
    owners_keys = jax.random.split(jax.random.fold_in(key_list[2], 1), ANCH // ROWS)
    owners_turns = jax.random.permutation(jax.random.fold_in(key_list[2], 3), ANCH // ROWS)
    owners = jax.vmap(lambda own, number: shared_out(jax.random.fold_in(key_list[2], 2), own, number, ROWS, N_BLK, 1, CAP, 2))(owners_keys, owners_turns).reshape((ANCH, 1))
    key_rows = set_ends(jax.random.randint(key_list[3], (ANCH,), 0, STORE_ENTRY_TALLY), jax.random.fold_in(key_list[3], 1), 0, STORE_ENTRY_TALLY - 1).astype(jnp.int32)
    return {"anchors": anchors, "keys": keys, "owners": owners, "key_rows": key_rows}


sharpness_divisor = 0.07
tiny_term = 1e-06

def unit_rows(values):
    wide_vals = values.astype(jnp.float32)
    length = jnp.sqrt(lax.optimization_barrier(jnp.sum(wide_vals * wide_vals, axis=1, keepdims=True)) + tiny_term)
    return (wide_vals / length, length)

def unitize_derivative(unit_vec, length, grads):
    along_unit = lax.optimization_barrier(jnp.sum(unit_vec * grads, axis=1, keepdims=True))
    return (grads - unit_vec * along_unit) / length

def inner_dotted(left, right):
    return lax.dot_general(left, right, (((1,), (1,)), ((), ())), preferred_element_type=jnp.float32)

def cols_dot(left, right):
    return lax.dot_general(left, right, (((0,), (0,)), ((), ())), preferred_element_type=jnp.float32)

def reference(anchors, keys, owners, key_rows):
    unitized_entries, lookup_magnitude = unit_rows(keys)
    key_bank = unitized_entries.astype(jnp.bfloat16)
    bank_split = key_bank.reshape(N_BLK, STORE_ENTRY_TALLY, EMBED_WIDTH)
    blocks = anchors.shape[0] // ROWS
    anchor_blocks = anchors.reshape(blocks, ROWS, EMBED_WIDTH)
    pos_all = (owners[:, 0] * STORE_ENTRY_TALLY + key_rows).astype(jnp.int32).reshape(blocks, ROWS)
    block_ids = jnp.arange(blocks, dtype=jnp.int32)

    def one_block(grad_carry, inputs):
        distractor_store_derivatives, matching_derivative = grad_carry
        block_index, anchor_rows, pos_index = inputs
        unit_vec, length = unit_rows(anchor_rows)
        probe_vectors = unit_vec.astype(jnp.bfloat16)
        bank_ids = ((block_index % N_BLK + jnp.arange(STEPS + 1, dtype=jnp.int32)) % N_BLK).astype(jnp.int32)
        adjacent_store = bank_split[bank_ids].reshape((STEPS + 1) * STORE_ENTRY_TALLY, EMBED_WIDTH)
        matching_entries = key_bank[pos_index].astype(jnp.float32)
        matching_similarity = lax.optimization_barrier(jnp.sum(probe_vectors.astype(jnp.float32) * matching_entries, axis=1)) / sharpness_divisor
        similarity_matrix = inner_dotted(probe_vectors, adjacent_store) / sharpness_divisor
        totals = jnp.exp(matching_similarity) + lax.optimization_barrier(jnp.sum(jnp.exp(similarity_matrix), axis=1))
        losses = jnp.log(totals) - matching_similarity
        weights = (jnp.exp(similarity_matrix) / totals[:, None]).astype(jnp.bfloat16)
        matching_weight = jnp.exp(matching_similarity) / totals - 1.0
        distractor_entries = jnp.dot(weights, adjacent_store, preferred_element_type=jnp.float32)
        probe_derivative = (distractor_entries + matching_weight[:, None] * matching_entries) / sharpness_divisor
        grad_rows = unitize_derivative(unit_vec, length, probe_derivative)
        to_banks = cols_dot(weights, probe_vectors).reshape(STEPS + 1, STORE_ENTRY_TALLY, EMBED_WIDTH)
        distractor_store_derivatives = distractor_store_derivatives.at[bank_ids].add(to_banks)
        matching_derivative = matching_derivative.at[pos_index].add(matching_weight[:, None] * probe_vectors.astype(jnp.float32))
        return ((distractor_store_derivatives, matching_derivative), (losses, grad_rows))
    start = (jnp.zeros((N_BLK, STORE_ENTRY_TALLY, EMBED_WIDTH), jnp.float32), jnp.zeros((N_BLK * STORE_ENTRY_TALLY, EMBED_WIDTH), jnp.float32))
    (distractor_store_derivatives, matching_derivative), (losses, grad_rows) = lax.scan(one_block, start, (block_ids, anchor_blocks, pos_all))
    store_derivative = (distractor_store_derivatives.reshape(N_BLK * STORE_ENTRY_TALLY, EMBED_WIDTH) + matching_derivative) / sharpness_divisor
    lookup_derivative = unitize_derivative(unitized_entries, lookup_magnitude, store_derivative)
    return (losses.reshape(-1), grad_rows.reshape(-1, EMBED_WIDTH), lookup_derivative)
```

```python
import functools

import jax
import jax.numpy as jnp
from jax import lax
from jax.experimental import pallas as pl
from jax.experimental.pallas import tpu as pltpu
from jax.sharding import PartitionSpec as P

STEPS = 4
DIVISOR = 0.07
TINY = 1e-06
LOG2E = 1.4426950408889634


F32 = jnp.float32
BF16 = jnp.bfloat16
VMEM = pl.BlockSpec(memory_space=pltpu.VMEM)
SMEM = pl.BlockSpec(memory_space=pltpu.SMEM)


def call(body, outs, flops, *args, smem=1):
    return pl.pallas_call(
        body,
        out_shape=[jax.ShapeDtypeStruct(s, d) for s, d in outs],
        in_specs=[SMEM] * smem + [VMEM] * (len(args) - smem),
        out_specs=[VMEM] * len(outs),
        compiler_params=pltpu.CompilerParams(vmem_limit_bytes=48 * 1024 * 1024),
        cost_estimate=pl.CostEstimate(flops=flops, transcendentals=0, bytes_accessed=1 << 20),
    )(*args)


def unit(values):
    wide = values.astype(F32)
    length = jnp.sqrt(jnp.sum(wide * wide, axis=1, keepdims=True) + TINY)
    return wide / length, length


def nt_dot(left, right):
    return lax.dot_general(left, right, (((1,), (1,)), ((), ())), preferred_element_type=F32)


def tn_dot(left, right):
    return lax.dot_general(left, right, (((0,), (0,)), ((), ())), preferred_element_type=F32)


def nn_dot(left, right):
    return lax.dot_general(left, right, (((1,), (0,)), ((), ())), preferred_element_type=F32)


def normalize_body(x_ref, o_ref):
    o_ref[...] = unit(x_ref[...])[0].astype(BF16)


def first_key(info_ref, distance, bank_rows, peers):
    bank = (info_ref[1] + 2 * distance) % peers
    return bank * bank_rows


def scores_body(info_ref, *refs, distance, peers, curve, own_neg, par_neg, raw):
    pieces = 1 if raw else curve
    key_refs, refs = refs[:pieces], refs[pieces:]
    p_own, p_par, q_own, q_par, before = refs[:5]
    outs = list(refs[5:])
    stats, bank = outs.pop(0), outs.pop(0)
    e_own = outs.pop(0) if own_neg else None
    e_par = outs.pop(0) if par_neg else None
    bank_rows = bank.shape[0]
    rows = bank_rows // curve
    anchors = q_own.shape[0]
    base = first_key(info_ref, distance, bank_rows, peers)
    for turn in range(curve):
        start = (info_ref[0] ^ turn) * rows
        if raw:
            part = unit(key_refs[0][pl.ds(start, rows), :])[0].astype(BF16)
        else:
            part = key_refs[turn][...]
        bank[turn * rows : (turn + 1) * rows, :] = part
    from_own = 2 * distance % peers
    from_par = (2 * distance + 2 * info_ref[2] - 1 + peers) % peers
    sides = (
        (0, q_own, p_own, e_own, own_neg, None),
        (2, q_par, p_par, e_par, par_neg, from_par <= STEPS),
    )
    del from_own

    def side(row, q_ref, p_ref, e_ref, negative):
        total = jnp.zeros((1, anchors), F32)
        found = jnp.zeros((1, anchors), F32)
        for turn in range(curve):
            span = slice(turn * rows, (turn + 1) * rows)
            logits = nt_dot(bank[span, :], q_ref[...])
            ids = lax.broadcasted_iota(jnp.int32, (rows, anchors), 0) + (
                base + (info_ref[0] ^ turn) * rows
            )
            found = found + jnp.sum(jnp.where(ids == p_ref[...], logits, 0.0), axis=0, keepdims=True)
            if negative:
                grown = jnp.exp2(logits * (LOG2E / DIVISOR))
                total = total + jnp.sum(grown, axis=0, keepdims=True)
                e_ref[span, :] = grown.astype(BF16)
        stats[row : row + 1, :] = before[row : row + 1, :] + total
        stats[row + 1 : row + 2, :] = before[row + 1 : row + 2, :] + found * (1.0 / DIVISOR)

    for row, q_ref, p_ref, e_ref, negative, when in sides:
        if not negative or when is None:
            side(row, q_ref, p_ref, e_ref, negative)
        else:

            @pl.when(when)
            def _():
                side(row, q_ref, p_ref, e_ref, True)

            @pl.when(jnp.logical_not(when))
            def _():
                e_ref[...] = jnp.zeros_like(e_ref)
                side(row, q_ref, p_ref, e_ref, False)


def scalings(mine, other, row):
    score = mine[row + 1 : row + 2, :] + other[3 - row : 4 - row, :]
    grown = jnp.exp2(score * LOG2E)
    total = mine[row : row + 1, :] + other[2 - row : 3 - row, :] + grown
    inverse = 1.0 / total
    return inverse, grown * inverse - 1.0, total, score


def weights_of(e_ref, span, ids, p_ref, inverse, coef):
    hit = jnp.where(ids == p_ref[...], coef, 0.0)
    if e_ref is not None:
        hit = hit + e_ref[span, :].astype(F32) * inverse
    return hit.astype(BF16)


def bank_grad_body(info_ref, *refs, distance, peers, curve, own_neg, par_neg):
    p_own, p_par, q_own, q_par, mine, other = refs[:6]
    refs = list(refs[6:])
    e_own = refs.pop(0) if own_neg else None
    e_par = refs.pop(0) if par_neg else None
    outs = refs
    rows = outs[0].shape[0]
    anchors = q_own.shape[0]
    base = first_key(info_ref, distance, rows * curve, peers)
    scale_own = scalings(mine, other, 0)
    scale_par = scalings(mine, other, 2)
    for turn in range(curve - 1, -1, -1):
        span = slice(turn * rows, (turn + 1) * rows)
        ids = lax.broadcasted_iota(jnp.int32, (rows, anchors), 0) + (
            base + (info_ref[0] ^ turn) * rows
        )
        left = weights_of(e_own, span, ids, p_own, *scale_own[:2])
        right = weights_of(e_par, span, ids, p_par, *scale_par[:2])
        grad = nn_dot(left, q_own[...]) + nn_dot(right, q_par[...])
        outs[turn][...] = grad.astype(outs[turn].dtype)


def query_grad_body(info_ref, *refs, order, negatives, peers, curve, row):
    p_ref, mine, other = refs[:3]
    refs = list(refs[3:])
    banks = {d: refs.pop(0) for d in order}
    grown = {d: refs.pop(0) if negatives[d] else None for d in order}
    out = refs.pop(0)
    bank_rows = banks[order[0]].shape[0]
    rows = bank_rows // curve
    anchors = p_ref.shape[1]
    inverse, coef, _, _ = scalings(mine, other, row)
    for number, d in enumerate(order):
        base = first_key(info_ref, d, bank_rows, peers)
        parts = []
        for turn in range(curve):
            span = slice(turn * rows, (turn + 1) * rows)
            ids = lax.broadcasted_iota(jnp.int32, (rows, anchors), 0) + (
                base + (info_ref[0] ^ turn) * rows
            )
            parts.append(weights_of(grown[d], span, ids, p_ref, inverse, coef))
        grad = tn_dot(banks[d][...], jnp.concatenate(parts, axis=0))
        if number:
            out[...] += grad
        else:
            out[...] = grad


def anchor_body(x_ref, left, right, mine, other, out, loss):
    anchors = x_ref.shape[0]
    step = min(anchors, 256)
    for at in range(0, anchors, step):
        span = slice(at, at + step)
        unit_vec, length = unit(x_ref[span, :])
        grad = (left[:, span] + right[:, span]).T * (1.0 / DIVISOR)
        along = jnp.sum(unit_vec * grad, axis=1, keepdims=True)
        out[span, :] = (grad - unit_vec * along) / length
    _, _, total, score = scalings(mine, other, 0)
    loss[...] = jnp.log(total) - score


def key_body(x_ref, *refs):
    grads, out = refs[:-1], refs[-1]
    total = grads[0][...].astype(F32)
    for part in grads[1:]:
        total = total + part[...].astype(F32)
    grad = total * (1.0 / DIVISOR)
    unit_vec, length = unit(x_ref[...])
    along = jnp.sum(unit_vec * grad, axis=1, keepdims=True)
    out[...] = ((grad - unit_vec * along) / length).astype(out.dtype)


def add_body(*refs):
    grads, out = refs[:-1], refs[-1]
    total = grads[0][...].astype(F32)
    for part in grads[1:]:
        total = total + part[...].astype(F32)
    out[...] = total.astype(out.dtype)


def place_body(info_ref, *refs):
    parts, out = refs[:-1], refs[-1]
    rows = parts[0].shape[0]
    for turn, part in enumerate(parts):
        out[pl.ds((info_ref[0] ^ turn) * rows, rows), :] = part[...].astype(F32)


def shards(anchors, keys, owners, key_rows):
    anchor_rows, width = anchors.shape
    bank_rows = keys.shape[0]
    curve = lax.axis_size("curve")
    peers = lax.axis_size("blk")
    pairs = peers // 2
    rows = bank_rows // curve
    at_curve = lax.axis_index("curve")
    at_blk = lax.axis_index("blk")
    lane = jnp.arange(4, dtype=jnp.int32)
    info = jnp.where(lane == 0, at_curve, jnp.where(lane == 1, at_blk, at_blk % 2)).astype(jnp.int32)

    def across(x, turn):
        return lax.ppermute(x, "curve", [(i, i ^ turn) for i in range(curve)])

    def partner(x):
        return lax.ppermute(x, "blk", [(i, i ^ 1) for i in range(peers)])

    def from_ahead(x, distance):
        return lax.ppermute(x, "blk", [((i + 2 * distance) % peers, i) for i in range(peers)])

    def to_ahead(x, distance):
        return lax.ppermute(x, "blk", [(i, (i + 2 * distance) % peers) for i in range(peers)])

    far = sorted(range(1, pairs), key=lambda d: (min(d, pairs - d), d))
    neg_own = {d: 2 * d % peers <= STEPS for d in range(pairs)}
    neg_par = {d: min((2 * d - 1) % peers, (2 * d + 1) % peers) <= STEPS for d in range(pairs)}

    own_keys = lax.dynamic_slice_in_dim(keys, at_curve * rows, rows, 0)
    (piece,) = call(normalize_body, [((rows, width), BF16)], 1 << 20, own_keys, smem=0)
    arrived = {d: from_ahead(piece, d) for d in far}
    (queries,) = call(normalize_body, [((anchor_rows, width), BF16)], 1 << 20, anchors, smem=0)
    queries_par = partner(queries)
    positive = (owners[:, 0] * bank_rows + key_rows).reshape(1, anchor_rows)
    positive_par = partner(positive)
    shared = (positive, positive_par, queries, queries_par)

    stats = jnp.zeros((4, anchor_rows), F32)
    banks, own_grown, par_grown = {}, {}, {}
    for d in [0] + far:
        parts = [keys] if d == 0 else [arrived[d]] + [across(arrived[d], e) for e in range(1, curve)]
        outs = [((4, anchor_rows), F32), ((bank_rows, width), BF16)]
        outs += [((bank_rows, anchor_rows), BF16)] * (neg_own[d] + neg_par[d])
        results = call(
            functools.partial(
                scores_body,
                distance=d,
                peers=peers,
                curve=curve,
                own_neg=neg_own[d],
                par_neg=neg_par[d],
                raw=d == 0,
            ),
            outs,
            4 * bank_rows * anchor_rows * width,
            info,
            *parts,
            *shared,
            stats,
        )
        stats, banks[d] = results[:2]
        results = list(results[2:])
        if neg_own[d]:
            own_grown[d] = results.pop(0)
        if neg_par[d]:
            par_grown[d] = results.pop(0)
    other = partner(stats)

    returned = []
    for d in far[::-1] + [0]:
        extra = [own_grown[d]] if neg_own[d] else []
        extra += [par_grown[d]] if neg_par[d] else []
        parts = call(
            functools.partial(
                bank_grad_body,
                distance=d,
                peers=peers,
                curve=curve,
                own_neg=neg_own[d],
                par_neg=neg_par[d],
            ),
            [((rows, width), F32)] + [((rows, width), BF16)] * (curve - 1),
            4 * bank_rows * anchor_rows * width,
            info,
            *shared,
            stats,
            other,
            *extra,
        )
        parts = [parts[0]] + [across(parts[e], e) for e in range(1, curve)]
        if d:
            (summed,) = call(add_body, [((rows, width), BF16)], 1 << 20, *parts, smem=0)
            returned.append(to_ahead(summed, d))
        else:
            returned += parts

    def query_grad(row, p, grown, negatives):
        return call(
            functools.partial(
                query_grad_body,
                order=tuple(range(pairs)),
                negatives=negatives,
                peers=peers,
                curve=curve,
                row=row,
            ),
            [((width, anchor_rows), F32)],
            2 * pairs * bank_rows * anchor_rows * width,
            info,
            p,
            stats,
            other,
            *[banks[d] for d in range(pairs)],
            *[grown[d] for d in range(pairs) if negatives[d]],
        )[0]

    received = partner(query_grad(2, positive_par, par_grown, neg_par))
    kept = query_grad(0, positive, own_grown, neg_own)
    grad_anchors, losses = call(
        anchor_body,
        [((anchor_rows, width), F32), ((1, anchor_rows), F32)],
        1 << 22,
        anchors,
        kept,
        received,
        stats,
        other,
        smem=0,
    )

    (mine,) = call(key_body, [((rows, width), BF16)], 1 << 20, own_keys, *returned, smem=0)
    (lookup_derivative,) = call(
        place_body,
        [((bank_rows, width), F32)],
        1 << 20,
        info,
        mine,
        *[across(mine, e) for e in range(1, curve)],
    )
    return losses.reshape(anchor_rows), grad_anchors, lookup_derivative


def solution(mesh):
    return jax.shard_map(
        shards,
        mesh=mesh,
        in_specs=(
            P(("curve", "blk"), None),
            P("blk", None),
            P(("curve", "blk"), None),
            P(("curve", "blk")),
        ),
        out_specs=(P(("curve", "blk")), P(("curve", "blk"), None), P("blk", None)),
        check_vma=False,
    )
```

```python
import functools

import jax
import jax.numpy as jnp
from jax import lax
from jax.experimental import pallas as pl
from jax.experimental.pallas import tpu as pltpu
from jax.sharding import PartitionSpec as P

STEPS = 4
DIVISOR = 0.07
TINY = 1e-06
LOG2E = 1.4426950408889634


F32 = jnp.float32
BF16 = jnp.bfloat16
VMEM = pl.BlockSpec(memory_space=pltpu.VMEM)
ANY = pl.BlockSpec(memory_space=pl.ANY)
SMEM = pl.BlockSpec(memory_space=pltpu.SMEM)


def call(body, outs, flops, *args, smem=1, scratch=(), placed=()):
    return pl.pallas_call(
        body,
        out_shape=[jax.ShapeDtypeStruct(s, d) for s, d in outs],
        in_specs=[SMEM] * smem + [VMEM] * (len(args) - smem),
        out_specs=[ANY if i in placed else VMEM for i in range(len(outs))],
        scratch_shapes=list(scratch),
        compiler_params=pltpu.CompilerParams(vmem_limit_bytes=48 * 1024 * 1024),
        cost_estimate=pl.CostEstimate(flops=flops, transcendentals=0, bytes_accessed=1 << 20),
    )(*args)


def unit(values):
    wide = values.astype(F32)
    length = jnp.sqrt(jnp.sum(wide * wide, axis=1, keepdims=True) + TINY)
    return wide / length, length


def nt_dot(left, right):
    return lax.dot_general(left, right, (((1,), (1,)), ((), ())), preferred_element_type=F32)


def nn_dot(left, right):
    return lax.dot_general(left, right, (((1,), (0,)), ((), ())), preferred_element_type=F32)


def sizes(whole, most):
    step = min(whole, most)
    while whole % step:
        step -= 1
    return step


def span(index, step):
    return pl.ds(pl.multiple_of(index * step, step), step)


def loop(count, body):
    lax.fori_loop(0, count, lambda index, carry: (body(index), carry)[1], 0)


def normalize_body(x_ref, o_ref):
    rows = x_ref.shape[0]
    step = sizes(rows, 128)

    def some(index):
        o_ref[span(index, step), :] = unit(x_ref[span(index, step), :])[0].astype(BF16)

    loop(rows // step, some)


def first_key(info_ref, distance, bank_rows, peers):
    return (info_ref[1] + 2 * distance) % peers * bank_rows


def scores_body(info_ref, *refs, distance, peers, curve, own_neg, par_neg, raw):
    pieces = 1 if raw else curve
    key_refs, refs = refs[:pieces], list(refs[pieces:])
    p_own, p_par, q_own, q_par, before, stats, turned = refs[:7]
    bank, refs = refs[-1], refs[7:-1]
    e_own = refs.pop(0) if own_neg else None
    e_par = refs.pop(0) if par_neg else None
    bank_rows = bank.shape[0]
    anchors = q_own.shape[0]
    step = sizes(anchors, 256)
    if raw:
        part = sizes(bank_rows, 128)

        def some(index):
            at = span(index, part)
            bank[at, :] = unit(key_refs[0][at, :])[0].astype(BF16)

        loop(bank_rows // part, some)
    else:
        for turn, key_ref in enumerate(key_refs):
            bank[span(info_ref[0] ^ turn, key_ref.shape[0]), :] = key_ref[...]
    turned[...] = bank[...].T
    base = first_key(info_ref, distance, bank_rows, peers)

    def side(row, q_ref, p_ref, e_ref, negative):
        def some(index):
            at = span(index, step)
            logits = nt_dot(bank[...], q_ref[at, :])
            ids = lax.broadcasted_iota(jnp.int32, (bank_rows, step), 0)
            found = jnp.sum(
                jnp.where(ids == p_ref[:, at] - base, logits, 0.0), axis=0, keepdims=True
            )
            total = before[row : row + 1, at]
            if negative:
                grown = jnp.exp2(logits * (LOG2E / DIVISOR))
                total = total + jnp.sum(grown, axis=0, keepdims=True)
                e_ref[:, at] = grown.astype(BF16)
            stats[row : row + 1, at] = total
            stats[row + 1 : row + 2, at] = before[row + 1 : row + 2, at] + found * (1.0 / DIVISOR)

        loop(anchors // step, some)

    side(0, q_own, p_own, e_own, own_neg)
    if par_neg:
        negative = (2 * distance + 2 * info_ref[2] - 1 + peers) % peers <= STEPS

        @pl.when(negative)
        def _():
            side(2, q_par, p_par, e_par, True)

        @pl.when(jnp.logical_not(negative))
        def _():
            e_par[...] = jnp.zeros_like(e_par)
            side(2, q_par, p_par, e_par, False)

    else:
        side(2, q_par, p_par, e_par, False)


def scalings(mine, other, row, at=slice(None)):
    score = mine[row + 1 : row + 2, at] + other[3 - row : 4 - row, at]
    grown = jnp.exp2(score * LOG2E)
    total = mine[row : row + 1, at] + other[2 - row : 3 - row, at] + grown
    inverse = 1.0 / total
    return inverse, grown * inverse - 1.0, total, score


def weights_of(e_ref, at, bank_rows, place, inverse, coef):
    ids = lax.broadcasted_iota(jnp.int32, (bank_rows, place.shape[1]), 0)
    weights = jnp.where(ids == place, coef, 0.0)
    if e_ref is not None:
        weights = weights + e_ref[:, at].astype(F32) * inverse
    return weights.astype(BF16)


def bank_grad_body(info_ref, *refs, distances, peers, curve, own_neg, par_neg):
    p_own, p_par, q_own, q_par, mine, other = refs[:6]
    refs = list(refs[6:])
    e_own = {d: refs.pop(0) if own_neg[d] else None for d in distances}
    e_par = {d: refs.pop(0) if par_neg[d] else None for d in distances}
    outs, grads = refs[:-1], refs[-1]
    bank_rows = grads.shape[0]
    rows = bank_rows // curve
    anchors = q_own.shape[0]
    step = sizes(anchors, 512)
    for number, d in enumerate(distances):
        base = first_key(info_ref, d, bank_rows, peers)
        grads[...] = jnp.zeros_like(grads)

        def side(row, q_ref, p_ref, e_ref):
            def some(index):
                at = span(index, step)
                inverse, coef, _, _ = scalings(mine, other, row, at)
                weights = weights_of(e_ref, at, bank_rows, p_ref[:, at] - base, inverse, coef)
                grads[...] += nn_dot(weights, q_ref[at, :])

            loop(anchors // step, some)

        side(0, q_own, p_own, e_own[d])
        side(2, q_par, p_par, e_par[d])
        for turn in range(curve):
            cut = grads[span(info_ref[0] ^ turn, rows), :]
            outs[turn][number * rows : (number + 1) * rows, :] = cut.astype(outs[turn].dtype)


def query_grad(info_ref, banks, grown, p_ref, mine, other, at, peers, row):
    bank_rows = banks[0].shape[1]
    inverse, coef, _, _ = scalings(mine, other, row, at)
    total = None
    for d, bank in enumerate(banks):
        place = p_ref[:, at] - first_key(info_ref, d, bank_rows, peers)
        part = nn_dot(bank[...], weights_of(grown[d], at, bank_rows, place, inverse, coef))
        total = part if total is None else total + part
    return total


def partner_grad_body(info_ref, p_ref, mine, other, *refs, negatives, peers):
    refs = list(refs)
    banks = [refs.pop(0) for _ in negatives]
    grown = [refs.pop(0) if negative else None for negative in negatives]
    out = refs.pop(0)
    anchors = p_ref.shape[1]
    step = sizes(anchors, 256)

    def some(index):
        at = span(index, step)
        out[:, at] = query_grad(info_ref, banks, grown, p_ref, mine, other, at, peers, 2)

    loop(anchors // step, some)


def anchor_body(info_ref, p_ref, mine, other, x_ref, received, *refs, negatives, peers):
    refs = list(refs)
    banks = [refs.pop(0) for _ in negatives]
    grown = [refs.pop(0) if negative else None for negative in negatives]
    out, loss, held, sems = refs
    anchors = p_ref.shape[1]
    step = sizes(anchors, 256)

    def copy(index):
        return pltpu.make_async_copy(
            held.at[span(index, step), :], out.at[span(index, step), :], sems.at[index]
        )

    def some(index):
        at = span(index, step)
        grad = query_grad(info_ref, banks, grown, p_ref, mine, other, at, peers, 0)
        grad = (grad + received[:, at]).T * (1.0 / DIVISOR)
        unit_vec, length = unit(x_ref[at, :])
        along = jnp.sum(unit_vec * grad, axis=1, keepdims=True)
        held[at, :] = (grad - unit_vec * along) / length
        copy(index).start()

    loop(anchors // step, some)
    _, _, total, score = scalings(mine, other, 0)
    loss[...] = jnp.log(total) - score
    loop(anchors // step, lambda index: copy(index).wait())


def key_body(x_ref, *refs):
    grads, out = refs[:-1], refs[-1]
    total = grads[0][...].astype(F32)
    for part in grads[1:]:
        total = total + part[...].astype(F32)
    grad = total * (1.0 / DIVISOR)
    unit_vec, length = unit(x_ref[...])
    along = jnp.sum(unit_vec * grad, axis=1, keepdims=True)
    out[...] = ((grad - unit_vec * along) / length).astype(out.dtype)


def add_body(*refs, count):
    grads, outs = refs[:-count], refs[-count:]
    rows = outs[0].shape[0]
    for number, out in enumerate(outs):
        at = slice(number * rows, (number + 1) * rows)
        total = grads[0][at, :].astype(F32)
        for part in grads[1:]:
            total = total + part[at, :].astype(F32)
        out[...] = total.astype(out.dtype)


def place_body(info_ref, *refs):
    parts, (out, held, sems) = refs[:-3], refs[-3:]
    rows = parts[0].shape[0]

    def copy(turn):
        at = span(info_ref[0] ^ turn, rows)
        return pltpu.make_async_copy(held.at[turn], out.at[at, :], sems.at[turn])

    for turn, part in enumerate(parts):
        held[turn] = part[...].astype(F32)
        copy(turn).start()
    for turn in range(len(parts)):
        copy(turn).wait()


def shards(anchors, keys, owners, key_rows):
    anchor_rows, width = anchors.shape
    bank_rows = keys.shape[0]
    curve = lax.axis_size("curve")
    peers = lax.axis_size("blk")
    pairs = peers // 2
    rows = bank_rows // curve
    at_curve = lax.axis_index("curve")
    at_blk = lax.axis_index("blk")
    lane = jnp.arange(4, dtype=jnp.int32)
    info = jnp.where(lane == 0, at_curve, jnp.where(lane == 1, at_blk, at_blk % 2)).astype(jnp.int32)
    block = 2 * bank_rows * anchor_rows * width

    def across(x):
        moved = [x]
        for turn in range(1, curve):
            moved.append(lax.ppermute(x, "curve", [(i, i ^ turn) for i in range(curve)]))
        return moved

    def exchange(parts):
        moved = [parts[0]]
        for turn in range(1, curve):
            route = [(i, i ^ turn) for i in range(curve)]
            moved.append(lax.ppermute(parts[turn], "curve", route))
        return moved

    def partner(x):
        return lax.ppermute(x, "blk", [(i, i ^ 1) for i in range(peers)])

    def from_ahead(x, distance):
        return lax.ppermute(x, "blk", [((i + 2 * distance) % peers, i) for i in range(peers)])

    def to_ahead(x, distance):
        return lax.ppermute(x, "blk", [(i, (i + 2 * distance) % peers) for i in range(peers)])

    far = far_order(pairs)
    neg_own = [2 * d % peers <= STEPS for d in range(pairs)]
    neg_par = [min((2 * d - 1) % peers, (2 * d + 1) % peers) <= STEPS for d in range(pairs)]

    own_keys = lax.dynamic_slice_in_dim(keys, at_curve * rows, rows, 0)
    (piece,) = call(normalize_body, [((rows, width), BF16)], 1 << 20, own_keys, smem=0)
    arrived = {d: from_ahead(piece, d) for d in far}
    (queries,) = call(normalize_body, [((anchor_rows, width), BF16)], 1 << 20, anchors, smem=0)
    queries_par = partner(queries)
    positive = (owners[:, 0] * bank_rows + key_rows).reshape(1, anchor_rows)
    positive_par = partner(positive)
    shared = (positive, positive_par, queries, queries_par)

    stats = jnp.zeros((4, anchor_rows), F32)
    banks, own_grown, par_grown = {}, {}, {}
    for d in [0] + far:
        parts = [keys] if d == 0 else across(arrived[d])
        outs = [((4, anchor_rows), F32), ((width, bank_rows), BF16)]
        outs += [((bank_rows, anchor_rows), BF16)] * (neg_own[d] + neg_par[d])
        results = call(
            functools.partial(
                scores_body,
                distance=d,
                peers=peers,
                curve=curve,
                own_neg=neg_own[d],
                par_neg=neg_par[d],
                raw=d == 0,
            ),
            outs,
            2 * block,
            info,
            *parts,
            *shared,
            stats,
            scratch=[pltpu.VMEM((bank_rows, width), BF16)],
        )
        stats, banks[d] = results[:2]
        results = list(results[2:])
        if neg_own[d]:
            own_grown[d] = results.pop(0)
        if neg_par[d]:
            par_grown[d] = results.pop(0)
    other = partner(stats)

    returned, final = [], []
    for group in grad_groups(pairs):
        parts = call(
            functools.partial(
                bank_grad_body,
                distances=group,
                peers=peers,
                curve=curve,
                own_neg=neg_own,
                par_neg=neg_par,
            ),
            [((len(group) * rows, width), F32)]
            + [((len(group) * rows, width), BF16)] * (curve - 1),
            2 * block * len(group),
            info,
            *shared,
            stats,
            other,
            *[own_grown[d] for d in group if neg_own[d]],
            *[par_grown[d] for d in group if neg_par[d]],
            scratch=[pltpu.VMEM((bank_rows, width), F32)],
        )
        parts = exchange(parts)
        if group == (0,):
            final = parts
            continue
        sums = call(
            functools.partial(add_body, count=len(group)),
            [((rows, width), BF16)] * len(group),
            1 << 20,
            *parts,
            smem=0,
        )
        returned += [to_ahead(x, d) for x, d in zip(sums, group)]

    own_banks = [banks[d] for d in range(pairs)]
    (sent,) = call(
        functools.partial(partner_grad_body, negatives=neg_par, peers=peers),
        [((width, anchor_rows), F32)],
        pairs * block,
        info,
        positive_par,
        stats,
        other,
        *own_banks,
        *[par_grown[d] for d in range(pairs) if neg_par[d]],
    )
    received = partner(sent)

    (mine,) = call(key_body, [((rows, width), BF16)], 1 << 20, own_keys, *final, *returned, smem=0)
    step = sizes(anchor_rows, 256)
    grad_anchors, losses = call(
        functools.partial(anchor_body, negatives=neg_own, peers=peers),
        [((anchor_rows, width), F32), ((1, anchor_rows), F32)],
        pairs * block,
        info,
        positive,
        stats,
        other,
        anchors,
        received,
        *own_banks,
        *[own_grown[d] for d in range(pairs) if neg_own[d]],
        scratch=[
            pltpu.VMEM((anchor_rows, width), F32),
            pltpu.SemaphoreType.DMA((anchor_rows // step,)),
        ],
        placed=(0,),
    )
    (lookup_derivative,) = call(
        place_body,
        [((bank_rows, width), F32)],
        1 << 20,
        info,
        *across(mine),
        scratch=[pltpu.VMEM((curve, rows, width), F32), pltpu.SemaphoreType.DMA((curve,))],
        placed=(0,),
    )
    return losses.reshape(anchor_rows), grad_anchors, lookup_derivative


def far_order(pairs):
    return sorted(range(1, pairs), key=lambda d: (min(d, pairs - d), d))


def grad_groups(pairs):
    return [tuple(sorted({d, pairs - d})) for d in range(pairs // 2, 0, -1)] + [(0,)]


def solution(mesh):
    return jax.shard_map(
        shards,
        mesh=mesh,
        in_specs=(
            P(("curve", "blk"), None),
            P("blk", None),
            P(("curve", "blk"), None),
            P(("curve", "blk")),
        ),
        out_specs=(P(("curve", "blk")), P(("curve", "blk"), None), P("blk", None)),
        check_vma=False,
    )
```

```python
import functools

import jax
import jax.numpy as jnp
from jax import lax
from jax.experimental import pallas as pl
from jax.experimental.pallas import tpu as pltpu
from jax.sharding import PartitionSpec as P

STEPS = 4
DIVISOR = 0.07
TINY = 1e-06
LOG2E = 1.4426950408889634


F32 = jnp.float32
BF16 = jnp.bfloat16
VMEM = pl.BlockSpec(memory_space=pltpu.VMEM)
ANY = pl.BlockSpec(memory_space=pl.ANY)


def call(body, outs, flops, *args, scratch=(), placed=()):
    return pl.pallas_call(
        body,
        out_shape=[jax.ShapeDtypeStruct(s, d) for s, d in outs],
        in_specs=[VMEM] * len(args),
        out_specs=[ANY if i in placed else VMEM for i in range(len(outs))],
        scratch_shapes=list(scratch),
        compiler_params=pltpu.CompilerParams(vmem_limit_bytes=48 * 1024 * 1024),
        cost_estimate=pl.CostEstimate(flops=flops, transcendentals=0, bytes_accessed=1 << 20),
    )(*args)


def unit(values):
    wide = values.astype(F32)
    length = jnp.sqrt(jnp.sum(wide * wide, axis=1, keepdims=True) + TINY)
    return wide / length, length


def nt_dot(left, right):
    return lax.dot_general(left, right, (((1,), (1,)), ((), ())), preferred_element_type=F32)


def nn_dot(left, right):
    return lax.dot_general(left, right, (((1,), (0,)), ((), ())), preferred_element_type=F32)


def sizes(whole, most):
    step = min(whole, most)
    while whole % step:
        step -= 1
    return step


def span(index, step):
    if isinstance(index, int):
        return slice(index * step, (index + 1) * step)
    return pl.ds(pl.multiple_of(index * step, step), step)


def loop(count, body):
    for index in range(count):
        body(index)


def normalize_body(x_ref, o_ref):
    rows = x_ref.shape[0]
    step = sizes(rows, 128)

    def some(index):
        o_ref[span(index, step), :] = unit(x_ref[span(index, step), :])[0].astype(BF16)

    loop(rows // step, some)


def first_key(distance, bank_rows, peers):
    return (lax.axis_index("blk") + 2 * distance) % peers * bank_rows


def scores_body(*refs, distance, peers, curve, own_neg, par_neg, raw):
    pieces = 1 if raw else curve
    key_refs, refs = refs[:pieces], list(refs[pieces:])
    p_own, p_par, q_own, q_par, before, stats, turned = refs[:7]
    bank, refs = refs[-1], refs[7:-1]
    e_own = refs.pop(0) if own_neg else None
    e_par = refs.pop(0) if par_neg else None
    bank_rows = bank.shape[0]
    anchors = q_own.shape[0]
    step = sizes(anchors, 256)
    if raw:
        part = sizes(bank_rows, 128)

        def some(index):
            at = span(index, part)
            bank[at, :] = unit(key_refs[0][at, :])[0].astype(BF16)

        loop(bank_rows // part, some)
    else:
        for turn, key_ref in enumerate(key_refs):
            bank[span(lax.axis_index("curve") ^ turn, key_ref.shape[0]), :] = key_ref[...]
    turned[...] = bank[...].T
    base = first_key(distance, bank_rows, peers)

    def side(row, q_ref, p_ref, e_ref, negative):
        def some(index):
            at = span(index, step)
            logits = nt_dot(bank[...], q_ref[at, :])
            ids = lax.broadcasted_iota(jnp.int32, (bank_rows, step), 0)
            found = jnp.sum(
                jnp.where(ids == p_ref[:, at] - base, logits, 0.0), axis=0, keepdims=True
            )
            total = before[row : row + 1, at]
            if negative:
                grown = jnp.exp2(logits * (LOG2E / DIVISOR))
                total = total + jnp.sum(grown, axis=0, keepdims=True)
                e_ref[:, at] = grown.astype(BF16)
            stats[row : row + 1, at] = total
            stats[row + 1 : row + 2, at] = before[row + 1 : row + 2, at] + found * (1.0 / DIVISOR)

        loop(anchors // step, some)

    side(0, q_own, p_own, e_own, own_neg)
    if par_neg:
        negative = (2 * distance + 2 * (lax.axis_index("blk") % 2) - 1 + peers) % peers <= STEPS

        @pl.when(negative)
        def _():
            side(2, q_par, p_par, e_par, True)

        @pl.when(jnp.logical_not(negative))
        def _():
            e_par[...] = jnp.zeros_like(e_par)
            side(2, q_par, p_par, e_par, False)

    else:
        side(2, q_par, p_par, e_par, False)


def scalings(mine, other, row, at=slice(None)):
    score = mine[row + 1 : row + 2, at] + other[3 - row : 4 - row, at]
    grown = jnp.exp2(score * LOG2E)
    total = mine[row : row + 1, at] + other[2 - row : 3 - row, at] + grown
    inverse = 1.0 / total
    return inverse, grown * inverse - 1.0, total, score


def weights_of(e_ref, at, bank_rows, place, inverse, coef):
    ids = lax.broadcasted_iota(jnp.int32, (bank_rows, place.shape[1]), 0)
    weights = jnp.where(ids == place, coef, 0.0)
    if e_ref is not None:
        weights = weights + e_ref[:, at].astype(F32) * inverse
    return weights.astype(BF16)


def bank_grad_body(*refs, distances, peers, curve, own_neg, par_neg):
    p_own, p_par, q_own, q_par, mine, other = refs[:6]
    refs = list(refs[6:])
    e_own = {d: refs.pop(0) if own_neg[d] else None for d in distances}
    e_par = {d: refs.pop(0) if par_neg[d] else None for d in distances}
    outs, grads = refs[:-1], refs[-1]
    bank_rows = grads.shape[0]
    rows = bank_rows // curve
    anchors = q_own.shape[0]
    step = sizes(anchors, 512)
    for number, d in enumerate(distances):
        base = first_key(d, bank_rows, peers)
        grads[...] = jnp.zeros_like(grads)

        def side(row, q_ref, p_ref, e_ref):
            def some(index):
                at = span(index, step)
                inverse, coef, _, _ = scalings(mine, other, row, at)
                weights = weights_of(e_ref, at, bank_rows, p_ref[:, at] - base, inverse, coef)
                grads[...] += nn_dot(weights, q_ref[at, :])

            loop(anchors // step, some)

        side(0, q_own, p_own, e_own[d])
        side(2, q_par, p_par, e_par[d])
        for turn in range(curve):
            cut = grads[span(lax.axis_index("curve") ^ turn, rows), :]
            outs[turn][number * rows : (number + 1) * rows, :] = cut.astype(outs[turn].dtype)


def query_grad(banks, grown, p_ref, mine, other, at, peers, row):
    bank_rows = banks[0].shape[1]
    inverse, coef, _, _ = scalings(mine, other, row, at)
    total = None
    for d, bank in enumerate(banks):
        place = p_ref[:, at] - first_key(d, bank_rows, peers)
        part = nn_dot(bank[...], weights_of(grown[d], at, bank_rows, place, inverse, coef))
        total = part if total is None else total + part
    return total


def partner_grad_body(p_ref, mine, other, *refs, negatives, peers):
    refs = list(refs)
    banks = [refs.pop(0) for _ in negatives]
    grown = [refs.pop(0) if negative else None for negative in negatives]
    out = refs.pop(0)
    anchors = p_ref.shape[1]
    step = sizes(anchors, 256)

    def some(index):
        at = span(index, step)
        out[:, at] = query_grad(banks, grown, p_ref, mine, other, at, peers, 2)

    loop(anchors // step, some)


def anchor_body(p_ref, mine, other, x_ref, received, *refs, negatives, peers):
    refs = list(refs)
    banks = [refs.pop(0) for _ in negatives]
    grown = [refs.pop(0) if negative else None for negative in negatives]
    out, loss, held, sems = refs
    anchors = p_ref.shape[1]
    step = sizes(anchors, 256)

    def copy(index):
        return pltpu.make_async_copy(
            held.at[span(index, step), :], out.at[span(index, step), :], sems.at[index]
        )

    def some(index):
        at = span(index, step)
        grad = query_grad(banks, grown, p_ref, mine, other, at, peers, 0)
        grad = (grad + received[:, at]).T * (1.0 / DIVISOR)
        unit_vec, length = unit(x_ref[at, :])
        along = jnp.sum(unit_vec * grad, axis=1, keepdims=True)
        held[at, :] = (grad - unit_vec * along) / length
        copy(index).start()

    loop(anchors // step, some)
    _, _, total, score = scalings(mine, other, 0)
    loss[...] = jnp.log(total) - score
    loop(anchors // step, lambda index: copy(index).wait())


def key_body(x_ref, *refs):
    grads, out = refs[:-1], refs[-1]
    total = grads[0][...].astype(F32)
    for part in grads[1:]:
        total = total + part[...].astype(F32)
    grad = total * (1.0 / DIVISOR)
    unit_vec, length = unit(x_ref[...])
    along = jnp.sum(unit_vec * grad, axis=1, keepdims=True)
    out[...] = ((grad - unit_vec * along) / length).astype(out.dtype)


def add_body(*refs, count):
    grads, outs = refs[:-count], refs[-count:]
    rows = outs[0].shape[0]
    for number, out in enumerate(outs):
        at = slice(number * rows, (number + 1) * rows)
        total = grads[0][at, :].astype(F32)
        for part in grads[1:]:
            total = total + part[at, :].astype(F32)
        out[...] = total.astype(out.dtype)


def place_body(*refs):
    parts, (out, held, sems) = refs[:-3], refs[-3:]
    rows = parts[0].shape[0]

    def copy(turn):
        at = span(lax.axis_index("curve") ^ turn, rows)
        return pltpu.make_async_copy(held.at[turn], out.at[at, :], sems.at[turn])

    for turn, part in enumerate(parts):
        held[turn] = part[...].astype(F32)
        copy(turn).start()
    for turn in range(len(parts)):
        copy(turn).wait()


def shards(anchors, keys, owners, key_rows):
    anchor_rows, width = anchors.shape
    bank_rows = keys.shape[0]
    curve = lax.axis_size("curve")
    peers = lax.axis_size("blk")
    pairs = peers // 2
    rows = bank_rows // curve
    at_curve = lax.axis_index("curve")
    block = 2 * bank_rows * anchor_rows * width

    def across(x):
        moved = [x]
        for turn in range(1, curve):
            moved.append(lax.ppermute(x, "curve", [(i, i ^ turn) for i in range(curve)]))
        return moved

    def exchange(parts):
        moved = [parts[0]]
        for turn in range(1, curve):
            route = [(i, i ^ turn) for i in range(curve)]
            moved.append(lax.ppermute(parts[turn], "curve", route))
        return moved

    def partner(x):
        return lax.ppermute(x, "blk", [(i, i ^ 1) for i in range(peers)])

    def from_ahead(x, distance):
        return lax.ppermute(x, "blk", [((i + 2 * distance) % peers, i) for i in range(peers)])

    def to_ahead(x, distance):
        return lax.ppermute(x, "blk", [(i, (i + 2 * distance) % peers) for i in range(peers)])

    far = far_order(pairs)
    neg_own = [2 * d % peers <= STEPS for d in range(pairs)]
    neg_par = [min((2 * d - 1) % peers, (2 * d + 1) % peers) <= STEPS for d in range(pairs)]

    own_keys = lax.dynamic_slice_in_dim(keys, at_curve * rows, rows, 0)
    (piece,) = call(normalize_body, [((rows, width), BF16)], 1 << 20, own_keys)
    arrived = {d: from_ahead(piece, d) for d in far}
    (queries,) = call(normalize_body, [((anchor_rows, width), BF16)], 1 << 20, anchors)
    queries_par = partner(queries)
    positive = (owners[:, 0] * bank_rows + key_rows).reshape(1, anchor_rows)
    positive_par = partner(positive)
    shared = (positive, positive_par, queries, queries_par)

    stats = jnp.zeros((4, anchor_rows), F32)
    banks, own_grown, par_grown = {}, {}, {}
    for d in [0] + far:
        parts = [keys] if d == 0 else across(arrived[d])
        outs = [((4, anchor_rows), F32), ((width, bank_rows), BF16)]
        outs += [((bank_rows, anchor_rows), BF16)] * (neg_own[d] + neg_par[d])
        results = call(
            functools.partial(
                scores_body,
                distance=d,
                peers=peers,
                curve=curve,
                own_neg=neg_own[d],
                par_neg=neg_par[d],
                raw=d == 0,
            ),
            outs,
            2 * block,
            *parts,
            *shared,
            stats,
            scratch=[pltpu.VMEM((bank_rows, width), BF16)],
        )
        stats, banks[d] = results[:2]
        results = list(results[2:])
        if neg_own[d]:
            own_grown[d] = results.pop(0)
        if neg_par[d]:
            par_grown[d] = results.pop(0)
    other = partner(stats)

    returned, final = [], []
    for group in grad_groups(pairs):
        parts = call(
            functools.partial(
                bank_grad_body,
                distances=group,
                peers=peers,
                curve=curve,
                own_neg=neg_own,
                par_neg=neg_par,
            ),
            [((len(group) * rows, width), F32)]
            + [((len(group) * rows, width), BF16)] * (curve - 1),
            2 * block * len(group),
            *shared,
            stats,
            other,
            *[own_grown[d] for d in group if neg_own[d]],
            *[par_grown[d] for d in group if neg_par[d]],
            scratch=[pltpu.VMEM((bank_rows, width), F32)],
        )
        parts = exchange(parts)
        if group == (0,):
            final = parts
            continue
        sums = call(
            functools.partial(add_body, count=len(group)),
            [((rows, width), BF16)] * len(group),
            1 << 20,
            *parts,
        )
        returned += [to_ahead(x, d) for x, d in zip(sums, group)]

    own_banks = [banks[d] for d in range(pairs)]
    (sent,) = call(
        functools.partial(partner_grad_body, negatives=neg_par, peers=peers),
        [((width, anchor_rows), F32)],
        pairs * block,
        positive_par,
        stats,
        other,
        *own_banks,
        *[par_grown[d] for d in range(pairs) if neg_par[d]],
    )
    received = partner(sent)

    (mine,) = call(key_body, [((rows, width), BF16)], 1 << 20, own_keys, *final, *returned)
    step = sizes(anchor_rows, 256)
    grad_anchors, losses = call(
        functools.partial(anchor_body, negatives=neg_own, peers=peers),
        [((anchor_rows, width), F32), ((1, anchor_rows), F32)],
        pairs * block,
        positive,
        stats,
        other,
        anchors,
        received,
        *own_banks,
        *[own_grown[d] for d in range(pairs) if neg_own[d]],
        scratch=[
            pltpu.VMEM((anchor_rows, width), F32),
            pltpu.SemaphoreType.DMA((anchor_rows // step,)),
        ],
        placed=(0,),
    )
    (lookup_derivative,) = call(
        place_body,
        [((bank_rows, width), F32)],
        1 << 20,
        *across(mine),
        scratch=[pltpu.VMEM((curve, rows, width), F32), pltpu.SemaphoreType.DMA((curve,))],
        placed=(0,),
    )
    return losses.reshape(anchor_rows), grad_anchors, lookup_derivative


def far_order(pairs):
    return sorted(range(1, pairs), key=lambda d: (min(d, pairs - d), d))


def grad_groups(pairs):
    return [tuple(sorted({d, pairs - d})) for d in range(pairs // 2, 0, -1)] + [(0,)]


def solution(mesh):
    return jax.shard_map(
        shards,
        mesh=mesh,
        in_specs=(
            P(("curve", "blk"), None),
            P("blk", None),
            P(("curve", "blk"), None),
            P(("curve", "blk")),
        ),
        out_specs=(P(("curve", "blk")), P(("curve", "blk"), None), P("blk", None)),
        check_vma=False,
    )
```

```python
import functools

import jax
import jax.numpy as jnp
from jax import lax
from jax.experimental import pallas as pl
from jax.experimental.pallas import tpu as pltpu
from jax.sharding import PartitionSpec as P

STEPS = 4
DIVISOR = 0.07
TINY = 1e-06
LOG2E = 1.4426950408889634


F32 = jnp.float32
BF16 = jnp.bfloat16
VMEM = pl.BlockSpec(memory_space=pltpu.VMEM)
ANY = pl.BlockSpec(memory_space=pl.ANY)


def call(body, outs, flops, *args, scratch=(), placed=()):
    return pl.pallas_call(
        body,
        out_shape=[jax.ShapeDtypeStruct(s, d) for s, d in outs],
        in_specs=[VMEM] * len(args),
        out_specs=[ANY if i in placed else VMEM for i in range(len(outs))],
        scratch_shapes=list(scratch),
        compiler_params=pltpu.CompilerParams(vmem_limit_bytes=48 * 1024 * 1024),
        cost_estimate=pl.CostEstimate(flops=flops, transcendentals=0, bytes_accessed=1 << 20),
    )(*args)


def unit(values):
    wide = values.astype(F32)
    length = jnp.sqrt(jnp.sum(wide * wide, axis=1, keepdims=True) + TINY)
    return wide / length, length


def nt_dot(left, right):
    return lax.dot_general(left, right, (((1,), (1,)), ((), ())), preferred_element_type=F32)


def nn_dot(left, right):
    return lax.dot_general(left, right, (((1,), (0,)), ((), ())), preferred_element_type=F32)


def sizes(whole, most):
    step = min(whole, most)
    while whole % step:
        step -= 1
    return step


def span(index, step):
    if isinstance(index, int):
        return slice(index * step, (index + 1) * step)
    return pl.ds(pl.multiple_of(index * step, step), step)


def loop(count, body):
    for index in range(count):
        body(index)


def normalize_body(x_ref, o_ref):
    rows = x_ref.shape[0]
    step = sizes(rows, 128)

    def some(index):
        o_ref[span(index, step), :] = unit(x_ref[span(index, step), :])[0].astype(BF16)

    loop(rows // step, some)


def first_key(distance, bank_rows, peers):
    return (lax.axis_index("blk") + 2 * distance) % peers * bank_rows


def scores_body(*refs, distance, peers, curve, own_neg, par_neg, raw):
    pieces = 1 if raw else curve
    key_refs, refs = refs[:pieces], list(refs[pieces:])
    p_own, p_par, q_own, q_par, before, stats, turned = refs[:7]
    bank, refs = refs[-1], refs[7:-1]
    e_own = refs.pop(0) if own_neg else None
    e_par = refs.pop(0) if par_neg else None
    bank_rows = bank.shape[0]
    anchors = q_own.shape[0]
    step = sizes(anchors, 256)
    if raw:
        part = sizes(bank_rows, 128)

        def some(index):
            at = span(index, part)
            bank[at, :] = unit(key_refs[0][at, :])[0].astype(BF16)

        loop(bank_rows // part, some)
    else:
        for turn, key_ref in enumerate(key_refs):
            bank[span(lax.axis_index("curve") ^ turn, key_ref.shape[0]), :] = key_ref[...]
    turned[...] = bank[...].T
    base = first_key(distance, bank_rows, peers)

    def side(row, q_ref, p_ref, e_ref, negative):
        def some(index):
            at = span(index, step)
            logits = nt_dot(bank[...], q_ref[at, :])
            ids = lax.broadcasted_iota(jnp.int32, (bank_rows, step), 0)
            found = jnp.sum(
                jnp.where(ids == p_ref[:, at] - base, logits, 0.0), axis=0, keepdims=True
            )
            total = before[row : row + 1, at]
            if negative:
                grown = jnp.exp2(logits * (LOG2E / DIVISOR))
                total = total + jnp.sum(grown, axis=0, keepdims=True)
                e_ref[:, at] = grown.astype(BF16)
            stats[row : row + 1, at] = total
            stats[row + 1 : row + 2, at] = before[row + 1 : row + 2, at] + found * (1.0 / DIVISOR)

        loop(anchors // step, some)

    side(0, q_own, p_own, e_own, own_neg)
    if par_neg:
        negative = (2 * distance + 2 * (lax.axis_index("blk") % 2) - 1 + peers) % peers <= STEPS

        @pl.when(negative)
        def _():
            side(2, q_par, p_par, e_par, True)

        @pl.when(jnp.logical_not(negative))
        def _():
            e_par[...] = jnp.zeros_like(e_par)
            side(2, q_par, p_par, e_par, False)

    else:
        side(2, q_par, p_par, e_par, False)


def scalings(mine, other, row, at=slice(None)):
    score = mine[row + 1 : row + 2, at] + other[3 - row : 4 - row, at]
    grown = jnp.exp2(score * LOG2E)
    total = mine[row : row + 1, at] + other[2 - row : 3 - row, at] + grown
    inverse = 1.0 / total
    return inverse, grown * inverse - 1.0, total, score


def weights_of(e_ref, at, bank_rows, place, inverse, coef):
    ids = lax.broadcasted_iota(jnp.int32, (bank_rows, place.shape[1]), 0)
    weights = jnp.where(ids == place, coef, 0.0)
    if e_ref is not None:
        weights = weights + e_ref[:, at].astype(F32) * inverse
    return weights.astype(BF16)


def bank_grad_body(*refs, distances, peers, curve, own_neg, par_neg):
    p_own, p_par, q_own, q_par, mine, other = refs[:6]
    refs = list(refs[6:])
    e_own = {d: refs.pop(0) if own_neg[d] else None for d in distances}
    e_par = {d: refs.pop(0) if par_neg[d] else None for d in distances}
    grads = refs.pop()
    outs = [refs.pop(0) for _ in range(curve)]
    w_own = {d: refs.pop(0) if own_neg[d] else None for d in distances}
    w_par = {d: refs.pop(0) if par_neg[d] else None for d in distances}
    bank_rows = grads.shape[0]
    rows = bank_rows // curve
    anchors = q_own.shape[0]
    step = sizes(anchors, 512)
    for number, d in enumerate(distances):
        base = first_key(d, bank_rows, peers)
        grads[...] = jnp.zeros_like(grads)

        def side(row, q_ref, p_ref, e_ref, w_ref):
            def some(index):
                at = span(index, step)
                inverse, coef, _, _ = scalings(mine, other, row, at)
                weights = weights_of(e_ref, at, bank_rows, p_ref[:, at] - base, inverse, coef)
                if w_ref is not None:
                    w_ref[:, at] = weights
                grads[...] += nn_dot(weights, q_ref[at, :])

            loop(anchors // step, some)

        side(0, q_own, p_own, e_own[d], w_own[d])
        side(2, q_par, p_par, e_par[d], w_par[d])
        for turn in range(curve):
            cut = grads[span(lax.axis_index("curve") ^ turn, rows), :]
            outs[turn][number * rows : (number + 1) * rows, :] = cut.astype(outs[turn].dtype)


def query_grad_body(p_ref, mine, other, *refs, negatives, peers, row):
    refs = list(refs)
    banks = [refs.pop(0) for _ in negatives]
    kept = [refs.pop(0) if negative else None for negative in negatives]
    out = refs.pop(0)
    bank_rows = banks[0].shape[1]
    anchors = p_ref.shape[1]
    step = sizes(anchors, 256)

    def some(index):
        at = span(index, step)
        inverse, coef, _, _ = scalings(mine, other, row, at)
        total = None
        for d, bank in enumerate(banks):
            if kept[d] is None:
                place = p_ref[:, at] - first_key(d, bank_rows, peers)
                weights = weights_of(None, at, bank_rows, place, inverse, coef)
            else:
                weights = kept[d][:, at]
            part = nn_dot(bank[...], weights)
            total = part if total is None else total + part
        out[:, at] = total.astype(out.dtype)

    loop(anchors // step, some)


def anchor_body(mine, other, x_ref, left, right, out, loss, held, sems):
    anchors = x_ref.shape[0]
    step = sizes(anchors, 256)

    def copy(index):
        return pltpu.make_async_copy(
            held.at[span(index, step), :], out.at[span(index, step), :], sems.at[index]
        )

    def some(index):
        at = span(index, step)
        grad = (left[:, at] + right[:, at].astype(F32)).T * (1.0 / DIVISOR)
        unit_vec, length = unit(x_ref[at, :])
        along = jnp.sum(unit_vec * grad, axis=1, keepdims=True)
        held[at, :] = (grad - unit_vec * along) / length
        copy(index).start()

    loop(anchors // step, some)
    _, _, total, score = scalings(mine, other, 0)
    loss[...] = jnp.log(total) - score
    loop(anchors // step, lambda index: copy(index).wait())


def key_body(x_ref, *refs):
    grads, out = refs[:-1], refs[-1]
    total = grads[0][...].astype(F32)
    for part in grads[1:]:
        total = total + part[...].astype(F32)
    grad = total * (1.0 / DIVISOR)
    unit_vec, length = unit(x_ref[...])
    along = jnp.sum(unit_vec * grad, axis=1, keepdims=True)
    out[...] = ((grad - unit_vec * along) / length).astype(out.dtype)


def add_body(*refs, count):
    grads, outs = refs[:-count], refs[-count:]
    rows = outs[0].shape[0]
    for number, out in enumerate(outs):
        at = slice(number * rows, (number + 1) * rows)
        total = grads[0][at, :].astype(F32)
        for part in grads[1:]:
            total = total + part[at, :].astype(F32)
        out[...] = total.astype(out.dtype)


def place_body(*refs):
    parts, (out, held, sems) = refs[:-3], refs[-3:]
    rows = parts[0].shape[0]

    def copy(turn):
        at = span(lax.axis_index("curve") ^ turn, rows)
        return pltpu.make_async_copy(held.at[turn], out.at[at, :], sems.at[turn])

    for turn, part in enumerate(parts):
        held[turn] = part[...].astype(F32)
        copy(turn).start()
    for turn in range(len(parts)):
        copy(turn).wait()


def shards(anchors, keys, owners, key_rows):
    anchor_rows, width = anchors.shape
    bank_rows = keys.shape[0]
    curve = lax.axis_size("curve")
    peers = lax.axis_size("blk")
    pairs = peers // 2
    rows = bank_rows // curve
    at_curve = lax.axis_index("curve")
    block = 2 * bank_rows * anchor_rows * width

    def across(x):
        moved = [x]
        for turn in range(1, curve):
            moved.append(lax.ppermute(x, "curve", [(i, i ^ turn) for i in range(curve)]))
        return moved

    def exchange(parts):
        moved = [parts[0]]
        for turn in range(1, curve):
            route = [(i, i ^ turn) for i in range(curve)]
            moved.append(lax.ppermute(parts[turn], "curve", route))
        return moved

    def partner(x):
        return lax.ppermute(x, "blk", [(i, i ^ 1) for i in range(peers)])

    def from_ahead(x, distance):
        return lax.ppermute(x, "blk", [((i + 2 * distance) % peers, i) for i in range(peers)])

    def to_ahead(x, distance):
        return lax.ppermute(x, "blk", [(i, (i + 2 * distance) % peers) for i in range(peers)])

    far = far_order(pairs)
    neg_own = [2 * d % peers <= STEPS for d in range(pairs)]
    neg_par = [min((2 * d - 1) % peers, (2 * d + 1) % peers) <= STEPS for d in range(pairs)]

    own_keys = lax.dynamic_slice_in_dim(keys, at_curve * rows, rows, 0)
    (piece,) = call(normalize_body, [((rows, width), BF16)], 1 << 20, own_keys)
    arrived = {d: from_ahead(piece, d) for d in far}
    (queries,) = call(normalize_body, [((anchor_rows, width), BF16)], 1 << 20, anchors)
    queries_par = partner(queries)
    positive = (owners[:, 0] * bank_rows + key_rows).reshape(1, anchor_rows)
    positive_par = partner(positive)
    shared = (positive, positive_par, queries, queries_par)

    stats = jnp.zeros((4, anchor_rows), F32)
    banks, own_grown, par_grown = {}, {}, {}
    for d in [0] + far:
        parts = [keys] if d == 0 else across(arrived[d])
        outs = [((4, anchor_rows), F32), ((width, bank_rows), BF16)]
        outs += [((bank_rows, anchor_rows), BF16)] * (neg_own[d] + neg_par[d])
        results = call(
            functools.partial(
                scores_body,
                distance=d,
                peers=peers,
                curve=curve,
                own_neg=neg_own[d],
                par_neg=neg_par[d],
                raw=d == 0,
            ),
            outs,
            2 * block,
            *parts,
            *shared,
            stats,
            scratch=[pltpu.VMEM((bank_rows, width), BF16)],
        )
        stats, banks[d] = results[:2]
        results = list(results[2:])
        if neg_own[d]:
            own_grown[d] = results.pop(0)
        if neg_par[d]:
            par_grown[d] = results.pop(0)
    other = partner(stats)

    returned, final = [], []
    own_kept, par_kept = {}, {}
    for group in grad_groups(pairs):
        parts = call(
            functools.partial(
                bank_grad_body,
                distances=group,
                peers=peers,
                curve=curve,
                own_neg=neg_own,
                par_neg=neg_par,
            ),
            [((len(group) * rows, width), F32)]
            + [((len(group) * rows, width), BF16)] * (curve - 1)
            + [((bank_rows, anchor_rows), BF16)] * sum(neg_own[d] + neg_par[d] for d in group),
            2 * block * len(group),
            *shared,
            stats,
            other,
            *[own_grown[d] for d in group if neg_own[d]],
            *[par_grown[d] for d in group if neg_par[d]],
            scratch=[pltpu.VMEM((bank_rows, width), F32)],
        )
        weights = list(parts[curve:])
        own_kept.update({d: weights.pop(0) for d in group if neg_own[d]})
        par_kept.update({d: weights.pop(0) for d in group if neg_par[d]})
        parts = exchange(parts[:curve])
        if group == (0,):
            final = parts
            continue
        sums = call(
            functools.partial(add_body, count=len(group)),
            [((rows, width), BF16)] * len(group),
            1 << 20,
            *parts,
        )
        returned += [to_ahead(x, d) for x, d in zip(sums, group)]

    def query_grad(dtype, row, p, kept, negatives):
        return call(
            functools.partial(query_grad_body, negatives=negatives, peers=peers, row=row),
            [((width, anchor_rows), dtype)],
            pairs * block,
            p,
            stats,
            other,
            *[banks[d] for d in range(pairs)],
            *[kept[d] for d in range(pairs) if negatives[d]],
        )[0]

    sent = query_grad(F32, 2, positive_par, par_kept, neg_par)
    received = partner(sent)
    own_part = query_grad(F32, 0, positive, own_kept, neg_own)

    (mine,) = call(key_body, [((rows, width), BF16)], 1 << 20, own_keys, *final, *returned)
    step = sizes(anchor_rows, 256)
    grad_anchors, losses = call(
        anchor_body,
        [((anchor_rows, width), F32), ((1, anchor_rows), F32)],
        1 << 22,
        stats,
        other,
        anchors,
        own_part,
        received,
        scratch=[
            pltpu.VMEM((anchor_rows, width), F32),
            pltpu.SemaphoreType.DMA((anchor_rows // step,)),
        ],
        placed=(0,),
    )
    (lookup_derivative,) = call(
        place_body,
        [((bank_rows, width), F32)],
        1 << 20,
        *across(mine),
        scratch=[pltpu.VMEM((curve, rows, width), F32), pltpu.SemaphoreType.DMA((curve,))],
        placed=(0,),
    )
    return losses.reshape(anchor_rows), grad_anchors, lookup_derivative


def far_order(pairs):
    return sorted(range(1, pairs), key=lambda d: (min(d, pairs - d), d))


def grad_groups(pairs):
    return [tuple(sorted({d, pairs - d})) for d in range(pairs // 2, 0, -1)] + [(0,)]


def solution(mesh):
    return jax.shard_map(
        shards,
        mesh=mesh,
        in_specs=(
            P(("curve", "blk"), None),
            P("blk", None),
            P(("curve", "blk"), None),
            P(("curve", "blk")),
        ),
        out_specs=(P(("curve", "blk")), P(("curve", "blk"), None), P("blk", None)),
        check_vma=False,
    )
```

```python
import functools
import math

import jax
import jax.numpy as jnp
from jax import lax
from jax.experimental import pallas as pl
from jax.experimental.pallas import tpu as pltpu
from jax.sharding import PartitionSpec as P

STEPS = 4
DIVISOR = 0.07
TINY = 1e-06
SLACK = 4
LOG2E = 1.4426950408889634


F32 = jnp.float32
BF16 = jnp.bfloat16
VMEM = pl.BlockSpec(memory_space=pltpu.VMEM)
ANY = pl.BlockSpec(memory_space=pl.ANY)


def call(body, outs, flops, *args, scratch=(), placed=()):
    held = sum(math.prod(x.shape) * x.dtype.itemsize for x in args)
    held += sum(math.prod(shape) * jnp.dtype(dtype).itemsize for shape, dtype in outs)
    held += sum(math.prod(x.shape) * 4 for x in scratch if x.memory_space == pltpu.VMEM)
    return pl.pallas_call(
        body,
        out_shape=[jax.ShapeDtypeStruct(s, d) for s, d in outs],
        in_specs=[VMEM] * len(args),
        out_specs=[ANY if i in placed else VMEM for i in range(len(outs))],
        scratch_shapes=list(scratch),
        compiler_params=pltpu.CompilerParams(vmem_limit_bytes=held + (SLACK << 20)),
        cost_estimate=pl.CostEstimate(flops=flops, transcendentals=0, bytes_accessed=1 << 20),
    )(*args)


def unit(values):
    wide = values.astype(F32)
    length = jnp.sqrt(jnp.sum(wide * wide, axis=1, keepdims=True) + TINY)
    return wide / length, length


def nt_dot(left, right):
    return lax.dot_general(left, right, (((1,), (1,)), ((), ())), preferred_element_type=F32)


def nn_dot(left, right):
    return lax.dot_general(left, right, (((1,), (0,)), ((), ())), preferred_element_type=F32)


def sizes(whole, most):
    step = min(whole, most)
    while whole % step:
        step -= 1
    return step


def span(index, step):
    if isinstance(index, int):
        return slice(index * step, (index + 1) * step)
    return pl.ds(pl.multiple_of(index * step, step), step)


def loop(count, body):
    for index in range(count):
        body(index)


def normalize_body(x_ref, o_ref):
    rows = x_ref.shape[0]
    step = sizes(rows, 128)

    def some(index):
        o_ref[span(index, step), :] = unit(x_ref[span(index, step), :])[0].astype(BF16)

    loop(rows // step, some)


def cuts(bank_rows, curve):
    parts = min(2, curve.bit_length() - 1)
    size = bank_rows // parts
    return [(bit, bit * size, size // 2) for bit in range(parts)]


def own_cut(bit, start, rows):
    return pl.ds(start + (lax.axis_index("curve") >> bit) % 2 * rows, rows)


def other_cut(bit, start, rows):
    return pl.ds(start + (1 - (lax.axis_index("curve") >> bit) % 2) * rows, rows)


def pieces_body(keys_ref, piece_ref, near_ref, *, curve):
    rows = piece_ref.shape[0]
    at = span(lax.axis_index("curve"), rows)
    piece_ref[...] = unit(keys_ref[at, :])[0].astype(BF16)
    filled = 0
    for bit, start, half in cuts(keys_ref.shape[0], curve):
        part = unit(keys_ref[own_cut(bit, start, half), :])[0].astype(BF16)
        near_ref[filled : filled + half, :] = part
        filled += half


def first_key(distance, bank_rows, peers):
    return (lax.axis_index("blk") + 2 * distance) % peers * bank_rows


def scores_body(*refs, distance, bank_rows, peers, curve, own_neg, par_neg):
    near = cuts(bank_rows, curve) if distance == 1 else None
    pieces = 1 if distance == 0 else 1 + len(near) if near else curve
    key_refs, refs = refs[:pieces], list(refs[pieces:])
    p_own, p_par, q_own, q_par, before, stats, turned = refs[:7]
    bank, refs = refs[-1], refs[7:-1]
    e_own = refs.pop(0) if own_neg else None
    e_par = refs.pop(0) if par_neg else None
    anchors = q_own.shape[0]
    step = sizes(anchors, 256)
    if distance == 0:
        part = sizes(bank_rows, 128)

        def some(index):
            at = span(index, part)
            bank[at, :] = unit(key_refs[0][at, :])[0].astype(BF16)

        loop(bank_rows // part, some)
    elif near:
        filled = 0
        for part, key_ref in zip(near, key_refs[1:]):
            bank[own_cut(*part), :] = key_refs[0][filled : filled + part[2], :]
            bank[other_cut(*part), :] = key_ref[...]
            filled += part[2]
    else:
        for turn, key_ref in enumerate(key_refs):
            bank[span(lax.axis_index("curve") ^ turn, key_ref.shape[0]), :] = key_ref[...]
    turned[...] = bank[...].T
    base = first_key(distance, bank_rows, peers)

    def side(row, q_ref, p_ref, e_ref, negative):
        def some(index):
            at = span(index, step)
            logits = nt_dot(bank[...], q_ref[at, :])
            ids = lax.broadcasted_iota(jnp.int32, (bank_rows, step), 0)
            found = jnp.sum(
                jnp.where(ids == p_ref[:, at] - base, logits, 0.0), axis=0, keepdims=True
            )
            total = before[row : row + 1, at]
            if negative:
                grown = jnp.exp2(logits * (LOG2E / DIVISOR))
                total = total + jnp.sum(grown, axis=0, keepdims=True)
                e_ref[:, at] = grown.astype(BF16)
            stats[row : row + 1, at] = total
            stats[row + 1 : row + 2, at] = before[row + 1 : row + 2, at] + found * (1.0 / DIVISOR)

        loop(anchors // step, some)

    side(0, q_own, p_own, e_own, own_neg)
    if par_neg:
        negative = (2 * distance + 2 * (lax.axis_index("blk") % 2) - 1 + peers) % peers <= STEPS

        @pl.when(negative)
        def _():
            side(2, q_par, p_par, e_par, True)

        @pl.when(jnp.logical_not(negative))
        def _():
            e_par[...] = jnp.zeros_like(e_par)
            side(2, q_par, p_par, e_par, False)

    else:
        side(2, q_par, p_par, e_par, False)


def scalings(mine, other, row, at=slice(None)):
    score = mine[row + 1 : row + 2, at] + other[3 - row : 4 - row, at]
    grown = jnp.exp2(score * LOG2E)
    total = mine[row : row + 1, at] + other[2 - row : 3 - row, at] + grown
    inverse = 1.0 / total
    return inverse, grown * inverse - 1.0, total, score


def weights_of(e_ref, at, bank_rows, place, inverse, coef):
    ids = lax.broadcasted_iota(jnp.int32, (bank_rows, place.shape[1]), 0)
    weights = jnp.where(ids == place, coef, 0.0)
    if e_ref is not None:
        weights = weights + e_ref[:, at].astype(F32) * inverse
    return weights.astype(BF16)


def bank_grad_body(*refs, distances, peers, curve, own_neg, par_neg):
    p_own, p_par, q_own, q_par, mine, other = refs[:6]
    refs = list(refs[6:])
    e_own = {d: refs.pop(0) if own_neg[d] else None for d in distances}
    e_par = {d: refs.pop(0) if par_neg[d] else None for d in distances}
    grads = refs.pop()
    outs = refs
    bank_rows = grads.shape[0]
    rows = bank_rows // curve
    anchors = q_own.shape[0]
    step = sizes(anchors, 512)
    for number, d in enumerate(distances):
        base = first_key(d, bank_rows, peers)
        grads[...] = jnp.zeros_like(grads)

        def side(row, q_ref, p_ref, e_ref):
            def some(index):
                at = span(index, step)
                inverse, coef, _, _ = scalings(mine, other, row, at)
                weights = weights_of(e_ref, at, bank_rows, p_ref[:, at] - base, inverse, coef)
                grads[...] += nn_dot(weights, q_ref[at, :])

            loop(anchors // step, some)

        side(0, q_own, p_own, e_own[d])
        side(2, q_par, p_par, e_par[d])
        for turn in range(curve):
            cut = grads[span(lax.axis_index("curve") ^ turn, rows), :]
            outs[turn][number * rows : (number + 1) * rows, :] = cut.astype(outs[turn].dtype)


def query_grad_body(p_ref, mine, other, *refs, negatives, peers, row):
    refs = list(refs)
    banks = [refs.pop(0) for _ in negatives]
    grown = [refs.pop(0) if negative else None for negative in negatives]
    out = refs.pop(0)
    bank_rows = banks[0].shape[1]
    anchors = p_ref.shape[1]
    step = sizes(anchors, 256)

    def some(index):
        at = span(index, step)
        inverse, coef, _, _ = scalings(mine, other, row, at)
        total = None
        for d, bank in enumerate(banks):
            place = p_ref[:, at] - first_key(d, bank_rows, peers)
            part = nn_dot(bank[...], weights_of(grown[d], at, bank_rows, place, inverse, coef))
            total = part if total is None else total + part
        out[:, at] = total.astype(out.dtype)

    loop(anchors // step, some)


def anchor_body(mine, other, x_ref, left, right, out, loss, held, sems):
    anchors = x_ref.shape[0]
    step = sizes(anchors, 256)

    def copy(index):
        return pltpu.make_async_copy(
            held.at[span(index, step), :], out.at[span(index, step), :], sems.at[index]
        )

    def some(index):
        at = span(index, step)
        grad = (left[:, at] + right[:, at].astype(F32)).T * (1.0 / DIVISOR)
        unit_vec, length = unit(x_ref[at, :])
        along = jnp.sum(unit_vec * grad, axis=1, keepdims=True)
        held[at, :] = (grad - unit_vec * along) / length
        copy(index).start()

    loop(anchors // step, some)
    _, _, total, score = scalings(mine, other, 0)
    loss[...] = jnp.log(total) - score
    loop(anchors // step, lambda index: copy(index).wait())


def key_body(keys_ref, *refs):
    grads, out = refs[:-1], refs[-1]
    x = keys_ref[span(lax.axis_index("curve"), out.shape[0]), :]
    total = grads[0][...].astype(F32)
    for part in grads[1:]:
        total = total + part[...].astype(F32)
    grad = total * (1.0 / DIVISOR)
    unit_vec, length = unit(x)
    along = jnp.sum(unit_vec * grad, axis=1, keepdims=True)
    out[...] = ((grad - unit_vec * along) / length).astype(out.dtype)


def add_body(*refs, count):
    grads, outs = refs[:-count], refs[-count:]
    rows = outs[0].shape[0]
    for number, out in enumerate(outs):
        at = slice(number * rows, (number + 1) * rows)
        total = grads[0][at, :].astype(F32)
        for part in grads[1:]:
            total = total + part[at, :].astype(F32)
        out[...] = total.astype(out.dtype)


def place_body(*refs):
    parts, (out, held, sems) = refs[:-3], refs[-3:]
    rows = parts[0].shape[0]

    def copy(turn):
        at = span(lax.axis_index("curve") ^ turn, rows)
        return pltpu.make_async_copy(held.at[turn], out.at[at, :], sems.at[turn])

    for turn, part in enumerate(parts):
        held[turn] = part[...].astype(F32)
        copy(turn).start()
    for turn in range(len(parts)):
        copy(turn).wait()


def shards(anchors, keys, owners, key_rows):
    anchor_rows, width = anchors.shape
    bank_rows = keys.shape[0]
    curve = lax.axis_size("curve")
    peers = lax.axis_size("blk")
    pairs = peers // 2
    rows = bank_rows // curve
    block = 2 * bank_rows * anchor_rows * width

    def neighbour(x, turn):
        return lax.ppermute(x, "curve", [(i, i ^ turn) for i in range(curve)])

    def exchange(parts):
        rest = [neighbour(parts[turn], turn) for turn in range(1, curve)]
        return [parts[0], *rest]

    def across(x):
        return exchange([x] * curve)

    def partner(x):
        return lax.ppermute(x, "blk", [(i, i ^ 1) for i in range(peers)])

    def from_ahead(x, distance):
        return lax.ppermute(x, "blk", [((i + 2 * distance) % peers, i) for i in range(peers)])

    def to_ahead(x, distance):
        return lax.ppermute(x, "blk", [(i, (i + 2 * distance) % peers) for i in range(peers)])

    far = far_order(pairs)
    neg_own = [2 * d % peers <= STEPS for d in range(pairs)]
    neg_par = [min((2 * d - 1) % peers, (2 * d + 1) % peers) <= STEPS for d in range(pairs)]

    near = cuts(bank_rows, curve)
    piece, near_piece = call(
        functools.partial(pieces_body, curve=curve),
        [((rows, width), BF16), ((bank_rows // 2, width), BF16)],
        1 << 20,
        keys,
    )
    arrived = {d: from_ahead(near_piece if d == 1 else piece, d) for d in far}
    (queries,) = call(normalize_body, [((anchor_rows, width), BF16)], 1 << 20, anchors)
    queries_par = partner(queries)
    positive = (owners[:, 0] * bank_rows + key_rows).reshape(1, anchor_rows)
    positive_par = partner(positive)
    shared = (positive, positive_par, queries, queries_par)

    stats = jnp.zeros((4, anchor_rows), F32)
    banks, own_grown, par_grown = {}, {}, {}
    for d in [0] + far:
        if d == 0:
            parts = [keys]
        elif d == 1:
            parts, filled = [arrived[d]], 0
            for bit, _, half in near:
                sent = arrived[d][filled : filled + half]
                parts.append(neighbour(sent, 1 << bit))
                filled += half
        else:
            parts = across(arrived[d])
        outs = [((4, anchor_rows), F32), ((width, bank_rows), BF16)]
        outs += [((bank_rows, anchor_rows), BF16)] * (neg_own[d] + neg_par[d])
        results = call(
            functools.partial(
                scores_body,
                distance=d,
                peers=peers,
                curve=curve,
                own_neg=neg_own[d],
                par_neg=neg_par[d],
                bank_rows=bank_rows,
            ),
            outs,
            2 * block,
            *parts,
            *shared,
            stats,
            scratch=[pltpu.VMEM((bank_rows, width), BF16)],
        )
        stats, banks[d] = results[:2]
        results = list(results[2:])
        if neg_own[d]:
            own_grown[d] = results.pop(0)
        if neg_par[d]:
            par_grown[d] = results.pop(0)
    other = partner(stats)

    returned, final = [], []
    for group in grad_groups(pairs):
        parts = call(
            functools.partial(
                bank_grad_body,
                distances=group,
                peers=peers,
                curve=curve,
                own_neg=neg_own,
                par_neg=neg_par,
            ),
            [((len(group) * rows, width), F32)]
            + [((len(group) * rows, width), BF16)] * (curve - 1),
            2 * block * len(group),
            *shared,
            stats,
            other,
            *[own_grown[d] for d in group if neg_own[d]],
            *[par_grown[d] for d in group if neg_par[d]],
            scratch=[pltpu.VMEM((bank_rows, width), F32)],
        )
        parts = exchange(parts)
        if group == (0,):
            final = parts
            continue
        sums = call(
            functools.partial(add_body, count=len(group)),
            [((rows, width), BF16)] * len(group),
            1 << 20,
            *parts,
        )
        returned += [to_ahead(x, d) for x, d in zip(sums, group)]

    def query_grad(dtype, row, p, grown, negatives):
        return call(
            functools.partial(query_grad_body, negatives=negatives, peers=peers, row=row),
            [((width, anchor_rows), dtype)],
            pairs * block,
            p,
            stats,
            other,
            *[banks[d] for d in range(pairs)],
            *[grown[d] for d in range(pairs) if negatives[d]],
        )[0]

    sent = query_grad(BF16, 2, positive_par, par_grown, neg_par)
    received = partner(sent)
    own_part = query_grad(F32, 0, positive, own_grown, neg_own)

    (mine,) = call(key_body, [((rows, width), BF16)], 1 << 20, keys, *final, *returned)
    step = sizes(anchor_rows, 256)
    grad_anchors, losses = call(
        anchor_body,
        [((anchor_rows, width), F32), ((1, anchor_rows), F32)],
        1 << 22,
        stats,
        other,
        anchors,
        own_part,
        received,
        scratch=[
            pltpu.VMEM((anchor_rows, width), F32),
            pltpu.SemaphoreType.DMA((anchor_rows // step,)),
        ],
        placed=(0,),
    )
    (lookup_derivative,) = call(
        place_body,
        [((bank_rows, width), F32)],
        1 << 20,
        *across(mine),
        scratch=[pltpu.VMEM((curve, rows, width), F32), pltpu.SemaphoreType.DMA((curve,))],
        placed=(0,),
    )
    return losses.reshape(anchor_rows), grad_anchors, lookup_derivative


def far_order(pairs):
    return sorted(range(1, pairs), key=lambda d: (d == 1, min(d, pairs - d), d))


def grad_groups(pairs):
    return [tuple(sorted({d, pairs - d})) for d in range(pairs // 2, 0, -1)] + [(0,)]


def solution(mesh):
    return jax.shard_map(
        shards,
        mesh=mesh,
        in_specs=(
            P(("curve", "blk"), None),
            P("blk", None),
            P(("curve", "blk"), None),
            P(("curve", "blk")),
        ),
        out_specs=(P(("curve", "blk")), P(("curve", "blk"), None), P("blk", None)),
        check_vma=False,
    )
```

```python
import functools
import math

import jax
import jax.numpy as jnp
from jax import lax
from jax.experimental import pallas as pl
from jax.experimental.pallas import tpu as pltpu
from jax.sharding import PartitionSpec as P

STEPS = 4
DIVISOR = 0.07
TINY = 1e-06
SLACK = 4
LOG2E = 1.4426950408889634


F32 = jnp.float32
BF16 = jnp.bfloat16
VMEM = pl.BlockSpec(memory_space=pltpu.VMEM)
ANY = pl.BlockSpec(memory_space=pl.ANY)


def call(body, outs, flops, *args, scratch=(), placed=()):
    held = sum(math.prod(x.shape) * x.dtype.itemsize for x in args)
    held += sum(math.prod(shape) * jnp.dtype(dtype).itemsize for shape, dtype in outs)
    held += sum(math.prod(x.shape) * 4 for x in scratch if x.memory_space == pltpu.VMEM)
    return pl.pallas_call(
        body,
        out_shape=[jax.ShapeDtypeStruct(s, d) for s, d in outs],
        in_specs=[VMEM] * len(args),
        out_specs=[ANY if i in placed else VMEM for i in range(len(outs))],
        scratch_shapes=list(scratch),
        compiler_params=pltpu.CompilerParams(vmem_limit_bytes=held + (SLACK << 20)),
        cost_estimate=pl.CostEstimate(flops=flops, transcendentals=0, bytes_accessed=1 << 20),
    )(*args)


def unit(values):
    wide = values.astype(F32)
    length = jnp.sqrt(jnp.sum(wide * wide, axis=1, keepdims=True) + TINY)
    return wide / length, length


def nt_dot(left, right):
    return lax.dot_general(left, right, (((1,), (1,)), ((), ())), preferred_element_type=F32)


def nn_dot(left, right):
    return lax.dot_general(left, right, (((1,), (0,)), ((), ())), preferred_element_type=F32)


def sizes(whole, most):
    step = min(whole, most)
    while whole % step:
        step -= 1
    return step


def span(index, step):
    if isinstance(index, int):
        return slice(index * step, (index + 1) * step)
    return pl.ds(pl.multiple_of(index * step, step), step)


def loop(count, body):
    for index in range(count):
        body(index)


def normalize_body(x_ref, o_ref):
    rows = x_ref.shape[0]
    step = sizes(rows, 128)

    def some(index):
        o_ref[span(index, step), :] = unit(x_ref[span(index, step), :])[0].astype(BF16)

    loop(rows // step, some)


def first_key(distance, bank_rows, peers):
    return (lax.axis_index("blk") + 2 * distance) % peers * bank_rows


def scores_body(*refs, distance, peers, curve, own_neg, par_neg, raw):
    pieces = 1 if raw else curve
    key_refs, refs = refs[:pieces], list(refs[pieces:])
    p_own, p_par, q_own, q_par, before, stats, turned = refs[:7]
    bank, refs = refs[-1], refs[7:-1]
    e_own = refs.pop(0) if own_neg else None
    e_par = refs.pop(0) if par_neg else None
    bank_rows = bank.shape[0]
    anchors = q_own.shape[0]
    step = sizes(anchors, 256)
    if raw:
        part = sizes(bank_rows, 128)

        def some(index):
            at = span(index, part)
            bank[at, :] = unit(key_refs[0][at, :])[0].astype(BF16)

        loop(bank_rows // part, some)
    else:
        for turn, key_ref in enumerate(key_refs):
            bank[span(lax.axis_index("curve") ^ turn, key_ref.shape[0]), :] = key_ref[...]
    turned[...] = bank[...].T
    base = first_key(distance, bank_rows, peers)

    def side(row, q_ref, p_ref, e_ref, negative):
        def some(index):
            at = span(index, step)
            logits = nt_dot(bank[...], q_ref[at, :])
            ids = lax.broadcasted_iota(jnp.int32, (bank_rows, step), 0)
            found = jnp.sum(
                jnp.where(ids == p_ref[:, at] - base, logits, 0.0), axis=0, keepdims=True
            )
            total = before[row : row + 1, at]
            if negative:
                grown = jnp.exp2(logits * (LOG2E / DIVISOR))
                total = total + jnp.sum(grown, axis=0, keepdims=True)
                e_ref[:, at] = grown.astype(BF16)
            stats[row : row + 1, at] = total
            stats[row + 1 : row + 2, at] = before[row + 1 : row + 2, at] + found * (1.0 / DIVISOR)

        loop(anchors // step, some)

    side(0, q_own, p_own, e_own, own_neg)
    if par_neg:
        negative = (2 * distance + 2 * (lax.axis_index("blk") % 2) - 1 + peers) % peers <= STEPS

        @pl.when(negative)
        def _():
            side(2, q_par, p_par, e_par, True)

        @pl.when(jnp.logical_not(negative))
        def _():
            e_par[...] = jnp.zeros_like(e_par)
            side(2, q_par, p_par, e_par, False)

    else:
        side(2, q_par, p_par, e_par, False)


def scalings(mine, other, row, at=slice(None)):
    score = mine[row + 1 : row + 2, at] + other[3 - row : 4 - row, at]
    grown = jnp.exp2(score * LOG2E)
    total = mine[row : row + 1, at] + other[2 - row : 3 - row, at] + grown
    inverse = 1.0 / total
    return inverse, grown * inverse - 1.0, total, score


def weights_of(e_ref, at, bank_rows, place, inverse, coef):
    ids = lax.broadcasted_iota(jnp.int32, (bank_rows, place.shape[1]), 0)
    weights = jnp.where(ids == place, coef, 0.0)
    if e_ref is not None:
        weights = weights + e_ref[:, at].astype(F32) * inverse
    return weights.astype(BF16)


def bank_grad_body(*refs, distances, peers, curve, own_neg, par_neg):
    p_own, p_par, q_own, q_par, mine, other = refs[:6]
    refs = list(refs[6:])
    e_own = {d: refs.pop(0) if own_neg[d] else None for d in distances}
    e_par = {d: refs.pop(0) if par_neg[d] else None for d in distances}
    grads = refs.pop()
    outs = refs
    bank_rows = grads.shape[0]
    rows = bank_rows // curve
    anchors = q_own.shape[0]
    step = sizes(anchors, 512)
    for number, d in enumerate(distances):
        base = first_key(d, bank_rows, peers)
        grads[...] = jnp.zeros_like(grads)

        def side(row, q_ref, p_ref, e_ref):
            def some(index):
                at = span(index, step)
                inverse, coef, _, _ = scalings(mine, other, row, at)
                weights = weights_of(e_ref, at, bank_rows, p_ref[:, at] - base, inverse, coef)
                grads[...] += nn_dot(weights, q_ref[at, :])

            loop(anchors // step, some)

        side(0, q_own, p_own, e_own[d])
        side(2, q_par, p_par, e_par[d])
        for turn in range(curve):
            cut = grads[span(lax.axis_index("curve") ^ turn, rows), :]
            outs[turn][number * rows : (number + 1) * rows, :] = cut.astype(outs[turn].dtype)


def query_grad_body(p_ref, mine, other, *refs, negatives, peers, row):
    refs = list(refs)
    banks = [refs.pop(0) for _ in negatives]
    grown = [refs.pop(0) if negative else None for negative in negatives]
    out = refs.pop(0)
    bank_rows = banks[0].shape[1]
    anchors = p_ref.shape[1]
    step = sizes(anchors, 256)

    def some(index):
        at = span(index, step)
        inverse, coef, _, _ = scalings(mine, other, row, at)
        total = None
        for d, bank in enumerate(banks):
            place = p_ref[:, at] - first_key(d, bank_rows, peers)
            part = nn_dot(bank[...], weights_of(grown[d], at, bank_rows, place, inverse, coef))
            total = part if total is None else total + part
        out[:, at] = total.astype(out.dtype)

    loop(anchors // step, some)


def anchor_body(mine, other, x_ref, left, right, out, loss, held, sems):
    anchors = x_ref.shape[0]
    step = sizes(anchors, 256)

    def copy(index):
        return pltpu.make_async_copy(
            held.at[span(index, step), :], out.at[span(index, step), :], sems.at[index]
        )

    def some(index):
        at = span(index, step)
        grad = (left[:, at] + right[:, at].astype(F32)).T * (1.0 / DIVISOR)
        unit_vec, length = unit(x_ref[at, :])
        along = jnp.sum(unit_vec * grad, axis=1, keepdims=True)
        held[at, :] = (grad - unit_vec * along) / length
        copy(index).start()

    loop(anchors // step, some)
    _, _, total, score = scalings(mine, other, 0)
    loss[...] = jnp.log(total) - score
    loop(anchors // step, lambda index: copy(index).wait())


def key_body(x_ref, *refs):
    grads, out = refs[:-1], refs[-1]
    total = grads[0][...].astype(F32)
    for part in grads[1:]:
        total = total + part[...].astype(F32)
    grad = total * (1.0 / DIVISOR)
    unit_vec, length = unit(x_ref[...])
    along = jnp.sum(unit_vec * grad, axis=1, keepdims=True)
    out[...] = ((grad - unit_vec * along) / length).astype(out.dtype)


def add_body(*refs, count):
    grads, outs = refs[:-count], refs[-count:]
    rows = outs[0].shape[0]
    for number, out in enumerate(outs):
        at = slice(number * rows, (number + 1) * rows)
        total = grads[0][at, :].astype(F32)
        for part in grads[1:]:
            total = total + part[at, :].astype(F32)
        out[...] = total.astype(out.dtype)


def place_body(*refs):
    parts, (out, held, sems) = refs[:-3], refs[-3:]
    rows = parts[0].shape[0]

    def copy(turn):
        at = span(lax.axis_index("curve") ^ turn, rows)
        return pltpu.make_async_copy(held.at[turn], out.at[at, :], sems.at[turn])

    for turn, part in enumerate(parts):
        held[turn] = part[...].astype(F32)
        copy(turn).start()
    for turn in range(len(parts)):
        copy(turn).wait()


def shards(anchors, keys, owners, key_rows):
    anchor_rows, width = anchors.shape
    bank_rows = keys.shape[0]
    curve = lax.axis_size("curve")
    peers = lax.axis_size("blk")
    pairs = peers // 2
    rows = bank_rows // curve
    at_curve = lax.axis_index("curve")
    block = 2 * bank_rows * anchor_rows * width

    def across(x):
        moved = [x]
        for turn in range(1, curve):
            moved.append(lax.ppermute(x, "curve", [(i, i ^ turn) for i in range(curve)]))
        return moved

    def exchange(parts):
        moved = [parts[0]]
        for turn in range(1, curve):
            route = [(i, i ^ turn) for i in range(curve)]
            moved.append(lax.ppermute(parts[turn], "curve", route))
        return moved

    def partner(x):
        return lax.ppermute(x, "blk", [(i, i ^ 1) for i in range(peers)])

    def from_ahead(x, distance):
        return lax.ppermute(x, "blk", [((i + 2 * distance) % peers, i) for i in range(peers)])

    def to_ahead(x, distance):
        return lax.ppermute(x, "blk", [(i, (i + 2 * distance) % peers) for i in range(peers)])

    far = far_order(pairs)
    neg_own = [2 * d % peers <= STEPS for d in range(pairs)]
    neg_par = [min((2 * d - 1) % peers, (2 * d + 1) % peers) <= STEPS for d in range(pairs)]

    own_keys = lax.dynamic_slice_in_dim(keys, at_curve * rows, rows, 0)
    (piece,) = call(normalize_body, [((rows, width), BF16)], 1 << 20, own_keys)
    arrived = {d: from_ahead(piece, d) for d in far}
    (queries,) = call(normalize_body, [((anchor_rows, width), BF16)], 1 << 20, anchors)
    queries_par = partner(queries)
    positive = (owners[:, 0] * bank_rows + key_rows).reshape(1, anchor_rows)
    positive_par = partner(positive)
    shared = (positive, positive_par, queries, queries_par)

    stats = jnp.zeros((4, anchor_rows), F32)
    banks, own_grown, par_grown = {}, {}, {}
    for d in [0] + sorted(far):
        parts = [keys] if d == 0 else across(arrived[d])
        outs = [((4, anchor_rows), F32), ((width, bank_rows), BF16)]
        outs += [((bank_rows, anchor_rows), BF16)] * (neg_own[d] + neg_par[d])
        results = call(
            functools.partial(
                scores_body,
                distance=d,
                peers=peers,
                curve=curve,
                own_neg=neg_own[d],
                par_neg=neg_par[d],
                raw=d == 0,
            ),
            outs,
            2 * block,
            *parts,
            *shared,
            stats,
            scratch=[pltpu.VMEM((bank_rows, width), BF16)],
        )
        stats, banks[d] = results[:2]
        results = list(results[2:])
        if neg_own[d]:
            own_grown[d] = results.pop(0)
        if neg_par[d]:
            par_grown[d] = results.pop(0)
    other = partner(stats)

    returned, final = [], []
    for group in grad_groups(pairs):
        parts = call(
            functools.partial(
                bank_grad_body,
                distances=group,
                peers=peers,
                curve=curve,
                own_neg=neg_own,
                par_neg=neg_par,
            ),
            [((len(group) * rows, width), F32)]
            + [((len(group) * rows, width), BF16)] * (curve - 1),
            2 * block * len(group),
            *shared,
            stats,
            other,
            *[own_grown[d] for d in group if neg_own[d]],
            *[par_grown[d] for d in group if neg_par[d]],
            scratch=[pltpu.VMEM((bank_rows, width), F32)],
        )
        parts = exchange(parts)
        if group == (0,):
            final = parts
            continue
        sums = call(
            functools.partial(add_body, count=len(group)),
            [((rows, width), BF16)] * len(group),
            1 << 20,
            *parts,
        )
        returned += [to_ahead(x, d) for x, d in zip(sums, group)]

    def query_grad(dtype, row, p, grown, negatives):
        return call(
            functools.partial(query_grad_body, negatives=negatives, peers=peers, row=row),
            [((width, anchor_rows), dtype)],
            pairs * block,
            p,
            stats,
            other,
            *[banks[d] for d in range(pairs)],
            *[grown[d] for d in range(pairs) if negatives[d]],
        )[0]

    sent = query_grad(BF16, 2, positive_par, par_grown, neg_par)
    received = partner(sent)
    own_part = query_grad(F32, 0, positive, own_grown, neg_own)

    (mine,) = call(key_body, [((rows, width), BF16)], 1 << 20, own_keys, *final, *returned)
    step = sizes(anchor_rows, 256)
    grad_anchors, losses = call(
        anchor_body,
        [((anchor_rows, width), F32), ((1, anchor_rows), F32)],
        1 << 22,
        stats,
        other,
        anchors,
        own_part,
        received,
        scratch=[
            pltpu.VMEM((anchor_rows, width), F32),
            pltpu.SemaphoreType.DMA((anchor_rows // step,)),
        ],
        placed=(0,),
    )
    (lookup_derivative,) = call(
        place_body,
        [((bank_rows, width), F32)],
        1 << 20,
        *across(mine),
        scratch=[pltpu.VMEM((curve, rows, width), F32), pltpu.SemaphoreType.DMA((curve,))],
        placed=(0,),
    )
    return losses.reshape(anchor_rows), grad_anchors, lookup_derivative


def far_order(pairs):
    return sorted(range(1, pairs), key=lambda d: (min(d, pairs - d), d))


def grad_groups(pairs):
    return [tuple(sorted({d, pairs - d})) for d in range(pairs // 2, 0, -1)] + [(0,)]


def solution(mesh):
    return jax.shard_map(
        shards,
        mesh=mesh,
        in_specs=(
            P(("curve", "blk"), None),
            P("blk", None),
            P(("curve", "blk"), None),
            P(("curve", "blk")),
        ),
        out_specs=(P(("curve", "blk")), P(("curve", "blk"), None), P("blk", None)),
        check_vma=False,
    )
```
